32 devices in a mesh: walker: 8 (over z, core), chol: 4 (over y, x).
Axes of the slice: x: 2, y: 2, z: 4, core: 2. Of those that a mesh axis runs over, the one named last changes fastest.
Arguments:
- chol_vectors: bfloat16 [256, 768, 192], P('chol', 'walker'), may hold values from -0.2 to 0.2, as said below
- green: bfloat16 [16, 768, 192], P('walker'), may hold values from -6 to 6
Outputs:
- energy: float32 [16], P('walker')
- gradient: float32 [16, 768, 192], P('walker', 'chol')
The draws below stay inside these ranges and needn't reach their ends.
Inputs may be any that keep to these rules, and one draw needn't show every extreme that they name: `chol_vectors`: independent entries of each vector; vector magnitudes differ from vector to vector.
All inputs are finite; a program needn't handle non-finite values.
Results may differ from the reference program's by a relative error of at most 0.0042.
Values may be sent and summed in bfloat16 or wider, within the bound.
A program may use at most 128 MiB of HBM per device.

```python
import jax
import jax.numpy as jnp
from jax import lax

M = 768
NOCC = 192
NCHOL = 256
WALKERS = 16


def draw_chol_vectors(key, part):
    index = jnp.arange(NCHOL, dtype=jnp.float32) / (NCHOL - 1)
    decay = 3.0 ** (-0.5 * index)
    values = jax.random.normal(key, (NCHOL, M, NOCC), jnp.float32)
    values = values * M ** (-0.5) * decay[:, None, None]
    return jnp.clip(values, -0.19921875, 0.19921875).astype(jnp.bfloat16)


def block_levels(rng, shape, pieces, least, high):
    def one(dim, shards_of):
        steps = jax.random.uniform(jax.random.fold_in(jax.random.fold_in(rng, 6), dim), (shards_of,), jnp.float32, least / len(pieces), high / len(pieces))
        return jnp.repeat(jnp.exp(steps), shape[dim] // shards_of).reshape((-1,) + (1,) * (len(shape) - dim - 1))

    loudness = one(*pieces[0])
    for cut in pieces[1:]:
        loudness = loudness * one(*cut)
    return loudness


def normal_values(rng, dims, scale, bound, cuts=(), kind=jnp.bfloat16):
    array = jax.random.normal(rng, dims, jnp.float32) * scale
    if len(cuts) > 0:
        array = block_levels(rng, dims, cuts, -0.22, 0.18) * array
    return jnp.clip(array, min=-bound, max=bound).astype(kind)


def setup_inputs(seed: int = 0) -> dict:
    key_list = jax.random.split(jax.random.key(seed), 3)
    chol_vectors = draw_chol_vectors(jax.random.fold_in(key_list[2], 71), 0)
    green = normal_values(key_list[1], (WALKERS, M, NOCC), 1.0, 6.0, ((0, 8),))
    return dict(chol_vectors=chol_vectors, green=green)


def reference(chol_vectors, green):
    factors = chol_vectors.astype(jnp.float32)
    escale = 1.0 / (NCHOL * NOCC)
    gscale = 1.0 / (NCHOL ** 0.5)

    def one_walker(single):
        gfloat = single.astype(jnp.float32)
        tmat = jnp.einsum("kmi,mj->kij", factors, gfloat, precision=lax.Precision.HIGHEST)
        energy = jnp.sum(tmat * jnp.swapaxes(tmat, 1, 2)) * escale
        tround = lax.optimization_barrier(tmat.astype(jnp.bfloat16)).astype(jnp.float32)
        gradient = jnp.einsum("kmi,kji->mj", factors, tround, precision=lax.Precision.HIGHEST) * gscale
        return energy, gradient

    energy, gradient = lax.map(one_walker, green)
    return energy, gradient
```

```python
import functools
import math

import jax
import jax.numpy as jnp
from jax import lax
from jax.experimental import pallas as pl
from jax.experimental.pallas import tpu as pltpu
from jax.sharding import PartitionSpec as P

MESH = pl.DeviceIdType.MESH
CORES = 2
ANY = pl.BlockSpec(memory_space=pl.ANY)


def remote(src, dst, send, recv, device):
    return pltpu.make_async_remote_copy(
        src_ref=src, dst_ref=dst, send_sem=send, recv_sem=recv, device_id=device, device_id_type=MESH
    )


def greet(devices):
    barrier = pltpu.get_barrier_semaphore()
    for device in devices:
        pl.semaphore_signal(barrier, inc=1, device_id=device, device_id_type=MESH)
    pl.semaphore_wait(barrier, len(devices))


def gather_kernel(
    span, groups, chol, green, blocks, greens, own_chol, own_green,
    chol_send, chol_recv, pair_send, pair_recv, green_send, green_recv, share_send, share_recv, local,
):
    walker, group = lax.axis_index("walker"), lax.axis_index("chol")
    chip, core = walker // CORES, walker % CORES
    kept, width = blocks.shape[1], green.shape[1] // groups
    partner = (chip * CORES + 1 - core, group)
    peers = [None] + [lax.rem(chip + d, span) for d in range(1, span)]
    sources = [None] + [lax.rem(chip - d + span, span) for d in range(1, span)]
    sides = [None] + [(walker, lax.rem(group + d, groups)) for d in range(1, groups)]
    greet([partner] + [(z * CORES + core, group) for z in peers[1:]] + sides[1:])

    mine = pl.ds(pl.multiple_of(group * width, math.gcd(width, 16)), width)
    waits = []
    first, quarters = [None], [None]
    for d in range(1, span):
        target = (peers[d] * CORES + core, group)
        quarter = remote(
            green.at[:, mine, :], greens.at[chip, :, mine, :], green_send.at[d], green_recv.at[d], target
        )
        quarter.start()
        quarters.append(quarter)
    for d in range(1, span):
        target = (peers[d] * CORES + core, group)
        block = remote(
            chol.at[pl.ds(peers[d] * kept, kept)], blocks.at[walker], chol_send.at[d], chol_recv.at[d], target
        )
        block.start()
        first.append(block)
    held = chol.at[pl.ds(chip * kept, kept)]
    pair = remote(held, blocks.at[walker], pair_send.at[0], pair_recv.at[0], partner)
    pair.start()
    waits.append(pair)
    takes = [pltpu.make_async_copy(held, own_chol, local.at[0]), pltpu.make_async_copy(green, own_green, local.at[1])]
    for take in takes:
        take.start()
    for take in takes:
        take.wait()
    puts = [
        pltpu.make_async_copy(own_chol, blocks.at[walker], local.at[2]),
        pltpu.make_async_copy(own_green, greens.at[chip], local.at[3]),
    ]
    for put in puts:
        put.start()
    for d in range(1, span):
        quarters[d].wait_recv()
        piece = greens.at[sources[d], :, mine, :]
        for e in range(1, groups):
            share = remote(piece, piece, share_send.at[d, e], share_recv.at[d, e], sides[e])
            share.start()
            waits.append(share)
    for d in range(1, span):
        first[d].wait_recv()
        landed = blocks.at[sources[d] * CORES + core]
        pair = remote(landed, landed, pair_send.at[d], pair_recv.at[d], partner)
        pair.start()
        waits.append(pair)
    for put in puts:
        put.wait()
    for d in range(1, span):
        quarters[d].wait_send()
        first[d].wait_send()
    for copy in waits:
        copy.wait()


def gather(span, groups, chol, green):
    kl, mb, width = chol.shape
    wl, m, _ = green.shape
    kept = kl // span
    dma = pltpu.SemaphoreType.DMA
    return pl.pallas_call(
        functools.partial(gather_kernel, span, groups),
        out_shape=(
            jax.ShapeDtypeStruct((span * CORES, kept, mb, width), chol.dtype),
            jax.ShapeDtypeStruct((span, wl, m, width), green.dtype),
        ),
        in_specs=[ANY, ANY],
        out_specs=(ANY, ANY),
        scratch_shapes=[
            pltpu.VMEM((kept, mb, width), chol.dtype),
            pltpu.VMEM((wl, m, width), green.dtype),
            dma((span,)), dma((span,)), dma((span,)), dma((span,)), dma((span,)), dma((span,)),
            dma((span, groups)), dma((span, groups)), dma((4,)),
        ],
        compiler_params=pltpu.CompilerParams(collective_id=0, has_side_effects=True),
    )(chol, green)


def product_kernel(chol, green, terms, energy, turned, total):
    k = pl.program_id(1)
    walkers = green.shape[0]

    @pl.when(k == 0)
    def _():
        total[...] = jnp.zeros_like(total)
        energy[...] = jnp.zeros_like(energy)

    turned[...] = chol[0].T
    per = math.gcd(walkers, 4)

    def step(n, carry):
        for u in range(per):
            w = n * per + u
            tmat = jnp.dot(turned[...], green[w], preferred_element_type=jnp.float32)
            energy[w] += jnp.sum(tmat * tmat.T, axis=0, keepdims=True)
            total[w] += lax.dot_general(
                chol[0], tmat.astype(jnp.bfloat16), (((1,), (1,)), ((), ())), preferred_element_type=jnp.float32
            )
        return carry

    lax.fori_loop(0, walkers // per, step, 0)

    @pl.when(k == pl.num_programs(1) - 1)
    def _():
        terms[...] = total[...].astype(terms.dtype)


def products(chol, green):
    kept, m, width = chol.shape
    walkers = green.shape[0]
    some = math.gcd(walkers, 8)
    return pl.pallas_call(
        product_kernel,
        out_shape=(
            jax.ShapeDtypeStruct((walkers, m, width), jnp.bfloat16),
            jax.ShapeDtypeStruct((walkers, 1, width), jnp.float32),
        ),
        grid=(walkers // some, kept),
        in_specs=[
            pl.BlockSpec((1, m, width), lambda g, k: (k, 0, 0)),
            pl.BlockSpec((some, m, width), lambda g, k: (g, 0, 0)),
        ],
        out_specs=(
            pl.BlockSpec((some, m, width), lambda g, k: (g, 0, 0)),
            pl.BlockSpec((some, 1, width), lambda g, k: (g, 0, 0)),
        ),
        scratch_shapes=[pltpu.VMEM((width, m), jnp.bfloat16), pltpu.VMEM((some, m, width), jnp.float32)],
        compiler_params=pltpu.CompilerParams(
            dimension_semantics=("arbitrary", "arbitrary"), vmem_limit_bytes=60 * 2**20
        ),
    )(chol, green)


def spread_kernel(span, groups, terms, energy, parts, energies, send, recv, esend, erecv):
    walker, group = lax.axis_index("walker"), lax.axis_index("chol")
    chip, core = walker // CORES, walker % CORES
    wl, width = parts.shape[1], parts.shape[2]
    others = [(d, e) for d in range(span) for e in range(groups) if d + e > 0]
    target = {(d, e): (lax.rem(chip + d, span), lax.rem(group + e, groups)) for d, e in others}
    greet([(target[o][0] * CORES + core, target[o][1]) for o in others])
    copies = []
    for n, o in enumerate(others):
        z, q = target[o]
        device = (z * CORES + core, q)
        block = terms.at[pl.ds(z * wl, wl), pl.ds(pl.multiple_of(q * width, math.gcd(width, 16)), width), :]
        copies.append(remote(block, parts.at[n], send.at[n], recv.at[n], device))
        copies.append(remote(energy.at[z], energies.at[n], esend.at[n], erecv.at[n], device))
    for copy in copies:
        copy.start()
    for copy in copies:
        copy.wait()


def spread(span, groups, terms, energy):
    walkers, m, width = terms.shape
    count = span * groups - 1
    dma = pltpu.SemaphoreType.DMA
    return pl.pallas_call(
        functools.partial(spread_kernel, span, groups),
        out_shape=(
            jax.ShapeDtypeStruct((count, walkers // span, m // groups, width), terms.dtype),
            jax.ShapeDtypeStruct((count,) + energy.shape[1:], energy.dtype),
        ),
        in_specs=[ANY, ANY],
        out_specs=(ANY, ANY),
        scratch_shapes=[dma((count,)), dma((count,)), dma((count,)), dma((count,))],
        compiler_params=pltpu.CompilerParams(collective_id=1, has_side_effects=True),
    )(terms, energy)


LANES = 128
HALF = LANES // 2
BATCH = 4


def flip(index, bits):
    for b in range(8):
        if (bits >> b) & 1:
            step = 1 << b
            index = index + step - 2 * step * lax.rem(lax.div(index, step), 2)
    return index


def join(left, right):
    return jnp.concatenate([left, right], axis=1)


def fused_kernel(
    span, groups, gscale, chol, green, out, energy,
    raw, packed, vectors, own, greens, turned, tmat, mixed, total, outgoing, incoming, last_out, last_in, lines, arrived,
    local, chol_send, chol_recv, pair_send, pair_recv, green_send, green_recv, share_send, share_recv,
    grad_send, grad_recv, last_send, last_recv, line_send, line_recv,
):
    walker, group = lax.axis_index("walker"), lax.axis_index("chol")
    chip, core = lax.div(walker, CORES), lax.rem(walker, CORES)
    kept, mb = raw.shape[1], raw.shape[2]
    m = total.shape[1]
    chunks = kept // BATCH
    quarter = m // groups
    part = quarter // 2
    cell = 3 * LANES
    bits = [1 << b for b in range(groups.bit_length() - 1)]
    orders = [bits, bits[::-1]]
    partner = (chip * CORES + 1 - core, group)

    def device(r, e):
        return (flip(chip, r) * CORES + core, flip(group, e))

    others = [(r, e) for r in range(span) for e in range(groups) if r + e > 0]
    barrier = pltpu.get_barrier_semaphore()
    for peer in [partner] + [device(r, e) for r, e in others]:
        pl.semaphore_signal(barrier, inc=1, device_id=peer, device_id_type=MESH)

    loads = [
        pltpu.make_async_copy(chol.at[pl.ds(flip(chip, r) * kept, kept)], raw.at[r], local.at[r]) for r in range(span)
    ]
    load_green = pltpu.make_async_copy(green, own, local.at[span])
    load_green.start()
    for r in reversed(range(span)):
        loads[r].start()

    load_green.wait()
    greens[3 * chip] = own[0, :, :LANES]
    greens[3 * chip + 1] = own[1, :, :LANES]
    greens[3 * chip + 2] = join(own[0, :, LANES:], own[1, :, LANES:])

    def pack(r, ch):
        pieces = []
        for p in range(BATCH // 2):
            a = raw[r, ch * BATCH + 2 * p]
            b = raw[r, ch * BATCH + 2 * p + 1]
            pieces += [a[:, :LANES], b[:, :LANES], join(a[:, LANES:], b[:, LANES:])]
        return pieces

    def pack_chunk(ch):
        for r in range(span):
            for n, piece in enumerate(pack(r, ch)):
                if r == 0:
                    vectors[ch, walker, :, n * LANES : (n + 1) * LANES] = piece
                else:
                    packed[r, ch, :, n * LANES : (n + 1) * LANES] = piece

    def chol_copy(ch, r):
        return remote(packed.at[r, ch], vectors.at[ch, walker], chol_send.at[ch, r], chol_recv.at[ch, r], device(r, 0))

    def pair_copy(ch, r):
        block = vectors.at[ch, flip(chip, r) * CORES + core]
        return remote(block, block, pair_send.at[ch, r], pair_recv.at[ch, r], partner)

    def green_piece(r, e):
        rows = pl.ds(pl.multiple_of(flip(group, e) * quarter, 16), quarter)
        return greens.at[pl.ds(3 * flip(chip, r), 3), rows, :]

    def green_copy(r, bit):
        n = r | bit
        return remote(green_piece(r, 0), green_piece(r, 0), green_send.at[n], green_recv.at[n], device(bit, 0))

    def share_copy(r, e):
        return remote(green_piece(r, 0), green_piece(r, 0), share_send.at[r, e], share_recv.at[r, e], device(0, e))

    for r in reversed(range(span)):
        loads[r].wait()
    pack_chunk(0)
    pl.semaphore_wait(barrier, len(others) + 1)

    highs = [1 << b for b in reversed(range(span.bit_length() - 1))]
    for bit in highs:
        green_copy(0, bit).start()
    for r in reversed(range(1, span)):
        chol_copy(0, r).start()
    pair_copy(0, 0).start()

    def pack_rest(ch, carry):
        pack_chunk(ch)
        return carry

    lax.fori_loop(1, chunks, pack_rest, 0)
    total[...] = jnp.zeros_like(total)

    for at, bit in enumerate(highs):
        done = [r for r in range(span) if r % (2 * bit) == 0]
        for r in done:
            n = r | bit
            green_copy(r, bit).wait_recv()
            for low in highs[at + 1 :]:
                green_copy(n, low).start()
            for e in range(1, groups):
                share_copy(n, e).start()

    def send_rest(ch, carry):
        for r in reversed(range(1, span)):
            chol_copy(ch, r).start()
        pair_copy(ch, 0).start()
        return carry

    lax.fori_loop(1, chunks, send_rest, 0)

    for r in range(1, span):
        for e in range(1, groups):
            share_copy(r, e).wait_recv()

    def turn(n, carry):
        turned[n] = greens[n].T
        return carry

    lax.fori_loop(0, 3 * span, turn, 0)

    def compute(ch, g):
        left = turned[pl.ds(6 * g, 6)].reshape(2 * cell, m)
        for n in range(3):
            cut = slice(2 * n * LANES, 2 * (n + 1) * LANES)
            right = vectors[ch, :, :, cut].reshape(m, 2 * LANES)
            tmat[:, cut] = jnp.dot(left, right, preferred_element_type=jnp.float32).astype(jnp.bfloat16)
        for k in range(2):
            for p in range(2):
                for at, size, step in ((0, LANES, LANES), (2 * LANES, HALF, HALF)):
                    source = [slice(p * cell + at + step * b, p * cell + at + step * b + size) for b in range(2)]
                    target = [slice(k * cell + at + step * a, k * cell + at + step * a + size) for a in range(2)]
                    for a in range(2):
                        for b in range(2):
                            mixed[target[a], p * cell + b * LANES : p * cell + (b + 1) * LANES] = tmat[
                                source[b], k * cell + a * LANES : k * cell + (a + 1) * LANES
                            ]
                    ends = [tmat[source[b], k * cell + 2 * LANES : (k + 1) * cell] for b in range(2)]
                    for a in range(2):
                        half = slice(a * HALF, (a + 1) * HALF)
                        mixed[target[a], p * cell + 2 * LANES : (p + 1) * cell] = join(ends[0][:, half], ends[1][:, half])
        whole = vectors[ch].reshape(m, 2 * cell)
        for n in range(3):
            sums = jnp.dot(
                whole, mixed[:, 2 * n * LANES : 2 * (n + 1) * LANES], preferred_element_type=jnp.float32
            )
            total[6 * g + 2 * n] += sums[:, :LANES]
            total[6 * g + 2 * n + 1] += sums[:, LANES:]

    def rows_of(e, colour):
        return pl.ds(pl.multiple_of(flip(group, e) * quarter + colour * part, 16), part)

    def held(r, e, colour):
        return total.at[pl.ds(3 * r, 3), rows_of(e, colour), :]

    def grad_copy(s, colour, e, bit):
        return remote(
            outgoing.at[s, colour, e], incoming.at[s, colour, e], grad_send.at[s, colour, e], grad_recv.at[s, colour, e],
            device(0, bit),
        )

    def first_step(s):
        for colour, order in enumerate(orders):
            for e in range(groups):
                if e & order[0]:
                    outgoing[s, colour, e] = held(s, e, colour)[...].astype(jnp.bfloat16)
        for colour, order in enumerate(orders):
            for e in range(groups):
                if e & order[0]:
                    grad_copy(s, colour, e, order[0]).start()

    def chunk_step(ch, carry):
        for r in reversed(range(1, span)):
            chol_copy(ch, r).wait_recv()
            pair_copy(ch, r).start()
        for r in range(span):
            pair_copy(ch, r).wait_recv()

        def group_step(n, carry):
            g = lax.rem(lax.div(chip, 2) + 1 + n, span // 2)
            compute(ch, g)

            @pl.when(ch == chunks - 1)
            def _():
                first_step(2 * g)
                first_step(2 * g + 1)

            return carry

        lax.fori_loop(0, span // 2, group_step, 0)
        return carry

    lax.fori_loop(0, chunks, chunk_step, 0)

    slots = [flip(chip, r) for r in reversed(range(span))]

    low = lax.broadcasted_iota(jnp.int32, (8, LANES), 1) < HALF

    def weigh(s, carry):
        def rows(n, sums):
            at = pl.ds(pl.multiple_of(n * 64, 64), 64)
            new = []
            for t in range(3):
                product = greens[3 * s + t, at, :].astype(jnp.float32) * total[3 * s + t, at, :]
                new.append(sums[t] + jnp.sum(product.reshape(8, 8, LANES), axis=0))
            return tuple(new)

        zero = jnp.zeros((8, LANES), jnp.float32)
        sums = lax.fori_loop(0, m // 64, rows, (zero, zero, zero))
        lines[s, 0] = sums[0] + jnp.where(low, sums[2], 0.0)
        lines[s, 1] = sums[1] + jnp.where(low, 0.0, sums[2])
        return carry

    lax.fori_loop(0, span, weigh, 0)

    def line_copy(n):
        r, e = others[n]
        return remote(lines.at[flip(chip, r)], arrived.at[n], line_send.at[n], line_recv.at[n], device(r, e))

    for n in range(len(others)):
        line_copy(n).start()

    def grad_step(s, at):
        for colour, order in enumerate(orders):
            past = sum(order[:at])
            bit = order[at]
            ready = [e for e in range(groups) if (e & bit) and not (e & past)]
            for e in ready:
                grad_copy(s, colour, e, bit).wait_recv()
                mine = e ^ bit
                piece = held(s, mine, colour)
                value = piece[...] + incoming[s, colour, e].astype(jnp.float32)
                if mine == 0:
                    piece[...] = value
                elif mine & order[at + 1]:
                    outgoing[s, colour, mine] = value.astype(jnp.bfloat16)
                    grad_copy(s, colour, mine, order[at + 1]).start()
                else:
                    piece[...] = value

    def last_copy(r):
        return remote(last_out.at[r], last_in.at[r], last_send.at[r], last_recv.at[r], device(r, 0))

    mine = pl.ds(pl.multiple_of(group * quarter, 16), quarter)

    def finish(n):
        r = span - 1 - n
        grad_step(slots[n], len(bits) - 1)
        if r > 0:
            last_out[r] = total[pl.ds(3 * slots[n], 3), mine, :].astype(jnp.bfloat16)
            last_copy(r).start()

    for at in range(len(bits) - 1):
        for n in range(span):
            grad_step(slots[n], at)
            if at == len(bits) - 2 and n > 1:
                finish(n - 2)
    for n in range(span - 2, span):
        finish(n)

    for r in range(1, span):
        last_copy(r).wait_recv()
    final = [total[3 * chip + t, mine, :] for t in range(3)]
    for r in range(1, span):
        final = [final[t] + last_in[r, t].astype(jnp.float32) for t in range(3)]
    final = [x * gscale for x in final]
    out[0, :, :LANES] = final[0]
    out[1, :, :LANES] = final[1]
    out[0, :, LANES:] = final[2][:, :HALF]
    out[1, :, LANES:] = final[2][:, HALF:]

    for n in range(len(others)):
        line_copy(n).wait_recv()
    sums = lines[chip]
    for n in range(len(others)):
        sums = sums + arrived[n]
    energy[...] = sums

    for bit in highs:
        for r in range(span):
            if r % (2 * bit) == 0:
                green_copy(r, bit).wait_send()
    for r in range(1, span):
        for e in range(1, groups):
            share_copy(r, e).wait_send()

    def drain(ch, carry):
        for r in range(1, span):
            chol_copy(ch, r).wait_send()
        for r in range(span):
            pair_copy(ch, r).wait_send()
        return carry

    lax.fori_loop(0, chunks, drain, 0)
    for s in range(span):
        for colour, order in enumerate(orders):
            for at, bit in enumerate(order):
                for e in range(groups):
                    if (e & bit) and not (e & sum(order[:at])):
                        grad_copy(s, colour, e, bit).wait_send()
    for r in range(1, span):
        last_copy(r).wait_send()
    for n in range(len(others)):
        line_copy(n).wait_send()


def fused(span, groups, gscale, chol, green):
    kl, mb, width = chol.shape
    wl, m, _ = green.shape
    kept = kl // span
    chunks = kept // BATCH
    quarter = m // groups
    count = span * groups - 1
    cell = 3 * LANES
    dma = pltpu.SemaphoreType.DMA
    half, full = jnp.bfloat16, jnp.float32
    return pl.pallas_call(
        functools.partial(fused_kernel, span, groups, gscale),
        out_shape=(
            jax.ShapeDtypeStruct((wl, quarter, width), full),
            jax.ShapeDtypeStruct((wl, 8, LANES), full),
        ),
        in_specs=[ANY, ANY],
        out_specs=(pl.BlockSpec(memory_space=pltpu.VMEM), pl.BlockSpec(memory_space=pltpu.VMEM)),
        scratch_shapes=[
            pltpu.VMEM((span, kept, mb, width), half),
            pltpu.VMEM((span, chunks, mb, 2 * cell), half),
            pltpu.VMEM((chunks, span * CORES, mb, 2 * cell), half),
            pltpu.VMEM((wl, m, width), half),
            pltpu.VMEM((3 * span, m, LANES), half),
            pltpu.VMEM((3 * span, LANES, m), half),
            pltpu.VMEM((2 * cell, 2 * cell), half),
            pltpu.VMEM((2 * cell, 2 * cell), half),
            pltpu.VMEM((3 * span, m, LANES), full),
            pltpu.VMEM((span, 2, groups, 3, quarter // 2, LANES), half),
            pltpu.VMEM((span, 2, groups, 3, quarter // 2, LANES), half),
            pltpu.VMEM((span, 3, quarter, LANES), half),
            pltpu.VMEM((span, 3, quarter, LANES), half),
            pltpu.VMEM((span, wl, 8, LANES), full),
            pltpu.VMEM((count, wl, 8, LANES), full),
            dma((span + 1,)),
            dma((chunks, span)), dma((chunks, span)), dma((chunks, span)), dma((chunks, span)),
            dma((span,)), dma((span,)), dma((span, groups)), dma((span, groups)),
            dma((span, 2, groups)), dma((span, 2, groups)), dma((span,)), dma((span,)), dma((count,)), dma((count,)),
        ],
        compiler_params=pltpu.CompilerParams(collective_id=2, has_side_effects=True, vmem_limit_bytes=60 * 2**20),
    )(chol, green)


def fits(span, groups, chol, green):
    kl, mb, width = chol.shape
    wl, m, _ = green.shape
    powers = span & (span - 1) == 0 and groups & (groups - 1) == 0
    tiles = width == LANES + HALF and wl == 2 and mb % 16 == 0 and m % 64 == 0 and m % (groups * 32) == 0
    return powers and tiles and span > 1 and groups > 2 and kl % (span * BATCH) == 0 and span * m * width <= 2**21


def per_device(span, groups, chol_vectors, green):
    kl, mb, width = chol_vectors.shape
    wl, m, _ = green.shape
    nchol = kl * groups
    escale = 1.0 / (nchol * width)
    gscale = 1.0 / nchol**0.5
    chip, group = lax.axis_index("walker") // CORES, lax.axis_index("chol")

    if fits(span, groups, chol_vectors, green):
        gradient, sums = fused(span, groups, gscale, chol_vectors, green)
        return jnp.sum(sums, axis=(1, 2)) * escale, gradient

    blocks, greens = gather(span, groups, chol_vectors, green)
    chol = jnp.transpose(blocks, (1, 0, 2, 3)).reshape(kl // span, m, width)
    terms, lines = products(chol, greens.reshape(span * wl, m, width))

    sums = jnp.sum(lines, axis=(1, 2)).reshape(span, wl, 1)
    sums = jnp.broadcast_to(sums, (span, wl, 128))
    parts, energies = spread(span, groups, terms, sums)
    own = lax.dynamic_slice(terms, (chip * wl, group * (m // groups), 0), (wl, m // groups, width))
    gradient = (own.astype(jnp.float32) + jnp.sum(parts.astype(jnp.float32), axis=0)) * gscale
    energy = lax.dynamic_index_in_dim(sums, chip, 0, keepdims=False) + jnp.sum(energies, axis=0)
    return energy[:, 0] * escale, gradient


def solution(mesh):
    span, groups = mesh.shape["walker"] // CORES, mesh.shape["chol"]
    return jax.shard_map(
        functools.partial(per_device, span, groups),
        mesh=mesh,
        in_specs=(P("chol", "walker", None), P("walker", None, None)),
        out_specs=(P("walker"), P("walker", "chol", None)),
        check_vma=False,
    )
```

```python
import functools
import math

import jax
import jax.numpy as jnp
from jax import lax
from jax.experimental import pallas as pl
from jax.experimental.pallas import tpu as pltpu
from jax.sharding import PartitionSpec as P

MESH = pl.DeviceIdType.MESH
CORES = 2
ANY = pl.BlockSpec(memory_space=pl.ANY)


def remote(src, dst, send, recv, device):
    return pltpu.make_async_remote_copy(
        src_ref=src, dst_ref=dst, send_sem=send, recv_sem=recv, device_id=device, device_id_type=MESH
    )


def greet(devices):
    barrier = pltpu.get_barrier_semaphore()
    for device in devices:
        pl.semaphore_signal(barrier, inc=1, device_id=device, device_id_type=MESH)
    pl.semaphore_wait(barrier, len(devices))


def gather_kernel(
    span, groups, chol, green, blocks, greens, own_chol, own_green,
    chol_send, chol_recv, pair_send, pair_recv, green_send, green_recv, share_send, share_recv, local,
):
    walker, group = lax.axis_index("walker"), lax.axis_index("chol")
    chip, core = walker // CORES, walker % CORES
    kept, width = blocks.shape[1], green.shape[1] // groups
    partner = (chip * CORES + 1 - core, group)
    peers = [None] + [lax.rem(chip + d, span) for d in range(1, span)]
    sources = [None] + [lax.rem(chip - d + span, span) for d in range(1, span)]
    sides = [None] + [(walker, lax.rem(group + d, groups)) for d in range(1, groups)]
    greet([partner] + [(z * CORES + core, group) for z in peers[1:]] + sides[1:])

    mine = pl.ds(pl.multiple_of(group * width, math.gcd(width, 16)), width)
    waits = []
    first, quarters = [None], [None]
    for d in range(1, span):
        target = (peers[d] * CORES + core, group)
        quarter = remote(
            green.at[:, mine, :], greens.at[chip, :, mine, :], green_send.at[d], green_recv.at[d], target
        )
        quarter.start()
        quarters.append(quarter)
    for d in range(1, span):
        target = (peers[d] * CORES + core, group)
        block = remote(
            chol.at[pl.ds(peers[d] * kept, kept)], blocks.at[walker], chol_send.at[d], chol_recv.at[d], target
        )
        block.start()
        first.append(block)
    held = chol.at[pl.ds(chip * kept, kept)]
    pair = remote(held, blocks.at[walker], pair_send.at[0], pair_recv.at[0], partner)
    pair.start()
    waits.append(pair)
    takes = [pltpu.make_async_copy(held, own_chol, local.at[0]), pltpu.make_async_copy(green, own_green, local.at[1])]
    for take in takes:
        take.start()
    for take in takes:
        take.wait()
    puts = [
        pltpu.make_async_copy(own_chol, blocks.at[walker], local.at[2]),
        pltpu.make_async_copy(own_green, greens.at[chip], local.at[3]),
    ]
    for put in puts:
        put.start()
    for d in range(1, span):
        quarters[d].wait_recv()
        piece = greens.at[sources[d], :, mine, :]
        for e in range(1, groups):
            share = remote(piece, piece, share_send.at[d, e], share_recv.at[d, e], sides[e])
            share.start()
            waits.append(share)
    for d in range(1, span):
        first[d].wait_recv()
        landed = blocks.at[sources[d] * CORES + core]
        pair = remote(landed, landed, pair_send.at[d], pair_recv.at[d], partner)
        pair.start()
        waits.append(pair)
    for put in puts:
        put.wait()
    for d in range(1, span):
        quarters[d].wait_send()
        first[d].wait_send()
    for copy in waits:
        copy.wait()


def gather(span, groups, chol, green):
    kl, mb, width = chol.shape
    wl, m, _ = green.shape
    kept = kl // span
    dma = pltpu.SemaphoreType.DMA
    return pl.pallas_call(
        functools.partial(gather_kernel, span, groups),
        out_shape=(
            jax.ShapeDtypeStruct((span * CORES, kept, mb, width), chol.dtype),
            jax.ShapeDtypeStruct((span, wl, m, width), green.dtype),
        ),
        in_specs=[ANY, ANY],
        out_specs=(ANY, ANY),
        scratch_shapes=[
            pltpu.VMEM((kept, mb, width), chol.dtype),
            pltpu.VMEM((wl, m, width), green.dtype),
            dma((span,)), dma((span,)), dma((span,)), dma((span,)), dma((span,)), dma((span,)),
            dma((span, groups)), dma((span, groups)), dma((4,)),
        ],
        compiler_params=pltpu.CompilerParams(collective_id=0, has_side_effects=True),
    )(chol, green)


def product_kernel(chol, green, terms, energy, turned, total):
    k = pl.program_id(1)
    walkers = green.shape[0]

    @pl.when(k == 0)
    def _():
        total[...] = jnp.zeros_like(total)
        energy[...] = jnp.zeros_like(energy)

    turned[...] = chol[0].T
    per = math.gcd(walkers, 4)

    def step(n, carry):
        for u in range(per):
            w = n * per + u
            tmat = jnp.dot(turned[...], green[w], preferred_element_type=jnp.float32)
            energy[w] += jnp.sum(tmat * tmat.T, axis=0, keepdims=True)
            total[w] += lax.dot_general(
                chol[0], tmat.astype(jnp.bfloat16), (((1,), (1,)), ((), ())), preferred_element_type=jnp.float32
            )
        return carry

    lax.fori_loop(0, walkers // per, step, 0)

    @pl.when(k == pl.num_programs(1) - 1)
    def _():
        terms[...] = total[...].astype(terms.dtype)


def products(chol, green):
    kept, m, width = chol.shape
    walkers = green.shape[0]
    some = math.gcd(walkers, 8)
    return pl.pallas_call(
        product_kernel,
        out_shape=(
            jax.ShapeDtypeStruct((walkers, m, width), jnp.bfloat16),
            jax.ShapeDtypeStruct((walkers, 1, width), jnp.float32),
        ),
        grid=(walkers // some, kept),
        in_specs=[
            pl.BlockSpec((1, m, width), lambda g, k: (k, 0, 0)),
            pl.BlockSpec((some, m, width), lambda g, k: (g, 0, 0)),
        ],
        out_specs=(
            pl.BlockSpec((some, m, width), lambda g, k: (g, 0, 0)),
            pl.BlockSpec((some, 1, width), lambda g, k: (g, 0, 0)),
        ),
        scratch_shapes=[pltpu.VMEM((width, m), jnp.bfloat16), pltpu.VMEM((some, m, width), jnp.float32)],
        compiler_params=pltpu.CompilerParams(
            dimension_semantics=("arbitrary", "arbitrary"), vmem_limit_bytes=60 * 2**20
        ),
    )(chol, green)


def spread_kernel(span, groups, terms, energy, parts, energies, send, recv, esend, erecv):
    walker, group = lax.axis_index("walker"), lax.axis_index("chol")
    chip, core = walker // CORES, walker % CORES
    wl, width = parts.shape[1], parts.shape[2]
    others = [(d, e) for d in range(span) for e in range(groups) if d + e > 0]
    target = {(d, e): (lax.rem(chip + d, span), lax.rem(group + e, groups)) for d, e in others}
    greet([(target[o][0] * CORES + core, target[o][1]) for o in others])
    copies = []
    for n, o in enumerate(others):
        z, q = target[o]
        device = (z * CORES + core, q)
        block = terms.at[pl.ds(z * wl, wl), pl.ds(pl.multiple_of(q * width, math.gcd(width, 16)), width), :]
        copies.append(remote(block, parts.at[n], send.at[n], recv.at[n], device))
        copies.append(remote(energy.at[z], energies.at[n], esend.at[n], erecv.at[n], device))
    for copy in copies:
        copy.start()
    for copy in copies:
        copy.wait()


def spread(span, groups, terms, energy):
    walkers, m, width = terms.shape
    count = span * groups - 1
    dma = pltpu.SemaphoreType.DMA
    return pl.pallas_call(
        functools.partial(spread_kernel, span, groups),
        out_shape=(
            jax.ShapeDtypeStruct((count, walkers // span, m // groups, width), terms.dtype),
            jax.ShapeDtypeStruct((count,) + energy.shape[1:], energy.dtype),
        ),
        in_specs=[ANY, ANY],
        out_specs=(ANY, ANY),
        scratch_shapes=[dma((count,)), dma((count,)), dma((count,)), dma((count,))],
        compiler_params=pltpu.CompilerParams(collective_id=1, has_side_effects=True),
    )(terms, energy)


LANES = 128
HALF = LANES // 2
BATCH = 4


def flip(index, bits):
    for b in range(8):
        if (bits >> b) & 1:
            step = 1 << b
            index = index + step - 2 * step * lax.rem(lax.div(index, step), 2)
    return index


def join(left, right):
    return jnp.concatenate([left, right], axis=1)


def fused_kernel(
    span, groups, escale, gscale, chol, green, out, energy,
    raw, packed, vectors, greens, turned, tmat, mixed, total, outgoing, incoming, last_out, last_in, lines, arrived,
    local, chol_send, chol_recv, pair_send, pair_recv, green_send, green_recv, share_send, share_recv,
    grad_send, grad_recv, last_send, last_recv, line_send, line_recv,
):
    walker, group = lax.axis_index("walker"), lax.axis_index("chol")
    chip, core = lax.div(walker, CORES), lax.rem(walker, CORES)
    kept, mb = raw.shape[1], raw.shape[2]
    m = total.shape[1]
    chunks = kept // BATCH
    quarter = m // groups
    part = quarter // 2
    cell = 3 * LANES
    bits = [1 << b for b in range(groups.bit_length() - 1)]
    orders = [bits, bits[::-1]]
    partner = (chip * CORES + 1 - core, group)

    def device(r, e):
        return (flip(chip, r) * CORES + core, flip(group, e))

    others = [(r, e) for r in range(span) for e in range(groups) if r + e > 0]
    barrier = pltpu.get_barrier_semaphore()
    for peer in [partner] + [device(r, e) for r, e in others]:
        pl.semaphore_signal(barrier, inc=1, device_id=peer, device_id_type=MESH)

    loads = [
        pltpu.make_async_copy(chol.at[pl.ds(flip(chip, r) * kept, kept)], raw.at[r], local.at[r]) for r in range(span)
    ]
    greens_in = []
    for w in range(CORES):
        for rows, tile, at in ((slice(0, LANES), w, 0), (slice(LANES, LANES + HALF), 2, w * HALF)):
            greens_in.append(
                pltpu.make_async_copy(
                    green.at[w, rows], turned.at[3 * chip + tile, at : at + rows.stop - rows.start], local.at[span + len(greens_in)]
                )
            )
    for copy in greens_in:
        copy.start()
    for r in reversed(range(span)):
        loads[r].start()

    def pack(r, ch):
        pieces = []
        for p in range(BATCH // 2):
            a = raw[r, ch * BATCH + 2 * p]
            b = raw[r, ch * BATCH + 2 * p + 1]
            pieces += [a[:, :LANES], b[:, :LANES], join(a[:, LANES:], b[:, LANES:])]
        return pieces

    def pack_chunk(ch):
        for r in range(span):
            for n, piece in enumerate(pack(r, ch)):
                if r == 0:
                    vectors[ch, walker, :, n * LANES : (n + 1) * LANES] = piece
                else:
                    packed[r, ch, :, n * LANES : (n + 1) * LANES] = piece

    def chol_copy(ch, r):
        return remote(packed.at[r, ch], vectors.at[ch, walker], chol_send.at[ch, r], chol_recv.at[ch, r], device(r, 0))

    def pair_copy(ch, r):
        block = vectors.at[ch, flip(chip, r) * CORES + core]
        return remote(block, block, pair_send.at[ch, r], pair_recv.at[ch, r], partner)

    def green_piece(r, e):
        size = LANES // groups
        rows = pl.ds(pl.multiple_of(flip(group, e) * size, 16), size)
        return turned.at[pl.ds(3 * flip(chip, r), 3), rows, :]

    def green_copy(r, bit):
        n = r | bit
        return remote(green_piece(r, 0), green_piece(r, 0), green_send.at[n], green_recv.at[n], device(bit, 0))

    def share_copy(r, e):
        return remote(green_piece(r, 0), green_piece(r, 0), share_send.at[r, e], share_recv.at[r, e], device(0, e))

    for copy in greens_in:
        copy.wait()
    for r in reversed(range(span)):
        loads[r].wait()
    pack_chunk(0)
    pl.semaphore_wait(barrier, len(others) + 1)

    highs = [1 << b for b in reversed(range(span.bit_length() - 1))]
    for bit in highs:
        green_copy(0, bit).start()
    for r in reversed(range(1, span)):
        chol_copy(0, r).start()
    pair_copy(0, 0).start()

    def pack_rest(ch, carry):
        pack_chunk(ch)
        return carry

    lax.fori_loop(1, chunks, pack_rest, 0)
    total[...] = jnp.zeros_like(total)

    for at, bit in enumerate(highs):
        done = [r for r in range(span) if r % (2 * bit) == 0]
        for r in done:
            n = r | bit
            green_copy(r, bit).wait_recv()
            for low in highs[at + 1 :]:
                green_copy(n, low).start()
            for e in range(1, groups):
                share_copy(n, e).start()

    def send_rest(ch, carry):
        for r in reversed(range(1, span)):
            chol_copy(ch, r).start()
        pair_copy(ch, 0).start()
        return carry

    lax.fori_loop(1, chunks, send_rest, 0)

    for r in range(1, span):
        for e in range(1, groups):
            share_copy(r, e).wait_recv()

    def turn(n, carry):
        greens[n] = turned[n].T
        return carry

    lax.fori_loop(0, 3 * span, turn, 0)

    def compute(ch, g):
        left = turned[pl.ds(6 * g, 6)].reshape(2 * cell, m)
        for n in range(3):
            cut = slice(2 * n * LANES, 2 * (n + 1) * LANES)
            right = vectors[ch, :, :, cut].reshape(m, 2 * LANES)
            tmat[:, cut] = jnp.dot(left, right, preferred_element_type=jnp.float32).astype(jnp.bfloat16)
        for k in range(2):
            for p in range(2):
                for at, size, step in ((0, LANES, LANES), (2 * LANES, HALF, HALF)):
                    source = [slice(p * cell + at + step * b, p * cell + at + step * b + size) for b in range(2)]
                    target = [slice(k * cell + at + step * a, k * cell + at + step * a + size) for a in range(2)]
                    for a in range(2):
                        for b in range(2):
                            mixed[target[a], p * cell + b * LANES : p * cell + (b + 1) * LANES] = tmat[
                                source[b], k * cell + a * LANES : k * cell + (a + 1) * LANES
                            ]
                    ends = [tmat[source[b], k * cell + 2 * LANES : (k + 1) * cell] for b in range(2)]
                    for a in range(2):
                        half = slice(a * HALF, (a + 1) * HALF)
                        mixed[target[a], p * cell + 2 * LANES : (p + 1) * cell] = join(ends[0][:, half], ends[1][:, half])
        whole = vectors[ch].reshape(m, 2 * cell)
        for n in range(3):
            sums = jnp.dot(
                whole, mixed[:, 2 * n * LANES : 2 * (n + 1) * LANES], preferred_element_type=jnp.float32
            )
            total[6 * g + 2 * n] += sums[:, :LANES]
            total[6 * g + 2 * n + 1] += sums[:, LANES:]

    def rows_of(e, colour):
        return pl.ds(pl.multiple_of(flip(group, e) * quarter + colour * part, 16), part)

    def held(r, e, colour):
        return total.at[pl.ds(3 * r, 3), rows_of(e, colour), :]

    def grad_copy(s, colour, e, bit):
        return remote(
            outgoing.at[s, colour, e], incoming.at[s, colour, e], grad_send.at[s, colour, e], grad_recv.at[s, colour, e],
            device(0, bit),
        )

    def ready(order, at):
        past = sum(order[:at])
        sent = [e for e in range(groups) if (e & order[at]) and not (e & past)]
        return sorted(sent, key=lambda e: e == order[at])

    def convert(s):
        for colour, order in enumerate(orders):
            for e in ready(order, 0):
                outgoing[s, colour, e] = held(s, e, colour)[...].astype(jnp.bfloat16)

    def send_first(s, n):
        for colour, order in enumerate(orders):
            grad_copy(s, colour, ready(order, 0)[n], order[0]).start()

    low = lax.broadcasted_iota(jnp.int32, (8, LANES), 1) < HALF
    top = lax.broadcasted_iota(jnp.int32, (8, LANES), 0)

    def weigh(s):
        def rows(n, sums):
            at = pl.ds(pl.multiple_of(n * 64, 64), 64)
            new = []
            for t in range(3):
                product = greens[3 * s + t, at, :].astype(jnp.float32) * total[3 * s + t, at, :]
                new.append(sums[t] + jnp.sum(product.reshape(8, 8, LANES), axis=0))
            return tuple(new)

        zero = jnp.zeros((8, LANES), jnp.float32)
        sums = lax.fori_loop(0, m // 64, rows, (zero, zero, zero))
        one = jnp.sum(sums[0] + jnp.where(low, sums[2], 0.0), axis=0, keepdims=True)
        two = jnp.sum(sums[1] + jnp.where(low, 0.0, sums[2]), axis=0, keepdims=True)
        lines[s] = jnp.where(top == 0, one, jnp.where(top == 1, two, 0.0))

    def chunk_step(ch, carry):
        for r in reversed(range(1, span)):
            chol_copy(ch, r).wait_recv()
            pair_copy(ch, r).start()
        for r in range(span):
            pair_copy(ch, r).wait_recv()

        def group_step(n, carry):
            g = lax.rem(lax.div(chip, 2) + 1 + n, span // 2)
            compute(ch, g)

            @pl.when(ch == chunks - 1)
            def _():
                convert(2 * g)
                convert(2 * g + 1)

            @pl.when((ch == chunks - 1) & (n == 0))
            def _():
                for r in (span - 1, span - 2):
                    for i in range(groups // 2):
                        send_first(flip(chip, r), i)

            @pl.when(ch == chunks - 1)
            def _():
                weigh(2 * g)
                weigh(2 * g + 1)

            return carry

        lax.fori_loop(0, span // 2, group_step, 0)
        return carry

    lax.fori_loop(0, chunks, chunk_step, 0)

    slots = [flip(chip, r) for r in range(span)]

    def line_copy(n):
        r, e = others[n]
        return remote(lines.at[slots[r]], arrived.at[n], line_send.at[n], line_recv.at[n], device(r, e))

    def take(r, at, n):
        s = slots[r]
        for colour, order in enumerate(orders):
            e = ready(order, at)[n]
            grad_copy(s, colour, e, order[at]).wait_recv()
            mine = e ^ order[at]
            piece = held(s, mine, colour)
            value = piece[...] + incoming[s, colour, e].astype(jnp.float32)
            if at + 1 < len(order) and mine & order[at + 1]:
                outgoing[s, colour, mine] = value.astype(jnp.bfloat16)
                grad_copy(s, colour, mine, order[at + 1]).start()
            else:
                piece[...] = value

    def last_copy(r):
        return remote(last_out.at[r], last_in.at[r], last_send.at[r], last_recv.at[r], device(r, 0))

    mine = pl.ds(pl.multiple_of(group * quarter, 16), quarter)

    def settle(r):
        take(r, 1, 0)
        if r > 0:
            last_out[r] = total[pl.ds(3 * slots[r], 3), mine, :].astype(jnp.bfloat16)
            last_copy(r).start()

    take(3, 0, 0)
    take(3, 0, 1)
    take(2, 0, 0)
    send_first(slots[1], 0)
    send_first(slots[1], 1)
    for n in range(len(others)):
        line_copy(n).start()
    take(2, 0, 1)
    settle(3)
    send_first(slots[0], 0)
    settle(2)
    take(1, 0, 0)
    send_first(slots[0], 1)
    take(1, 0, 1)
    take(0, 0, 0)
    settle(1)
    take(0, 0, 1)
    settle(0)

    for r in range(1, span):
        last_copy(r).wait_recv()
    final = [total[3 * chip + t, mine, :] for t in range(3)]
    for r in range(1, span):
        final = [final[t] + last_in[r, t].astype(jnp.float32) for t in range(3)]
    final = [x * gscale for x in final]
    out[0, :, :LANES] = final[0]
    out[1, :, :LANES] = final[1]
    out[0, :, LANES:] = final[2][:, :HALF]
    out[1, :, LANES:] = final[2][:, HALF:]

    for n in range(len(others)):
        line_copy(n).wait_recv()
    sums = lines[chip]
    for n in range(len(others)):
        sums = sums + arrived[n]
    for w in range(CORES):
        energy[w] = jnp.sum(jnp.where(top == w, sums, 0.0)) * escale

    for bit in highs:
        for r in range(span):
            if r % (2 * bit) == 0:
                green_copy(r, bit).wait_send()
    for r in range(1, span):
        for e in range(1, groups):
            share_copy(r, e).wait_send()

    def drain(ch, carry):
        for r in range(1, span):
            chol_copy(ch, r).wait_send()
        for r in range(span):
            pair_copy(ch, r).wait_send()
        return carry

    lax.fori_loop(0, chunks, drain, 0)
    for s in range(span):
        for colour, order in enumerate(orders):
            for at, bit in enumerate(order):
                for e in range(groups):
                    if (e & bit) and not (e & sum(order[:at])):
                        grad_copy(s, colour, e, bit).wait_send()
    for r in range(1, span):
        last_copy(r).wait_send()
    for n in range(len(others)):
        line_copy(n).wait_send()


def fused(span, groups, escale, gscale, chol, green):
    kl, mb, width = chol.shape
    wl, m, _ = green.shape
    kept = kl // span
    chunks = kept // BATCH
    quarter = m // groups
    count = span * groups - 1
    cell = 3 * LANES
    dma = pltpu.SemaphoreType.DMA
    half, full = jnp.bfloat16, jnp.float32
    return pl.pallas_call(
        functools.partial(fused_kernel, span, groups, escale, gscale),
        out_shape=(
            jax.ShapeDtypeStruct((wl, quarter, width), full),
            jax.ShapeDtypeStruct((wl,), full),
        ),
        in_specs=[ANY, ANY],
        out_specs=(pl.BlockSpec(memory_space=pltpu.VMEM), pl.BlockSpec(memory_space=pltpu.SMEM)),
        scratch_shapes=[
            pltpu.VMEM((span, kept, mb, width), half),
            pltpu.VMEM((span, chunks, mb, 2 * cell), half),
            pltpu.VMEM((chunks, span * CORES, mb, 2 * cell), half),
            pltpu.VMEM((3 * span, m, LANES), half),
            pltpu.VMEM((3 * span, LANES, m), half),
            pltpu.VMEM((2 * cell, 2 * cell), half),
            pltpu.VMEM((2 * cell, 2 * cell), half),
            pltpu.VMEM((3 * span, m, LANES), full),
            pltpu.VMEM((span, 2, groups, 3, quarter // 2, LANES), half),
            pltpu.VMEM((span, 2, groups, 3, quarter // 2, LANES), half),
            pltpu.VMEM((span, 3, quarter, LANES), half),
            pltpu.VMEM((span, 3, quarter, LANES), half),
            pltpu.VMEM((span, 8, LANES), full),
            pltpu.VMEM((count, 8, LANES), full),
            dma((span + 2 * wl,)),
            dma((chunks, span)), dma((chunks, span)), dma((chunks, span)), dma((chunks, span)),
            dma((span,)), dma((span,)), dma((span, groups)), dma((span, groups)),
            dma((span, 2, groups)), dma((span, 2, groups)), dma((span,)), dma((span,)), dma((count,)), dma((count,)),
        ],
        compiler_params=pltpu.CompilerParams(collective_id=2, has_side_effects=True, vmem_limit_bytes=60 * 2**20),
    )(chol, jnp.swapaxes(green, 1, 2))


def fits(span, groups, chol, green):
    kl, mb, width = chol.shape
    wl, m, _ = green.shape
    powers = span & (span - 1) == 0 and groups & (groups - 1) == 0
    tiles = width == LANES + HALF and wl == 2 and mb % 16 == 0 and m % 64 == 0 and m % (groups * 32) == 0
    return powers and tiles and span == 4 and groups == 4 and kl % (span * BATCH) == 0 and span * m * width <= 2**21


def per_device(span, groups, chol_vectors, green):
    kl, mb, width = chol_vectors.shape
    wl, m, _ = green.shape
    nchol = kl * groups
    escale = 1.0 / (nchol * width)
    gscale = 1.0 / nchol**0.5
    chip, group = lax.axis_index("walker") // CORES, lax.axis_index("chol")

    if fits(span, groups, chol_vectors, green):
        gradient, energy = fused(span, groups, escale, gscale, chol_vectors, green)
        return energy, gradient

    blocks, greens = gather(span, groups, chol_vectors, green)
    chol = jnp.transpose(blocks, (1, 0, 2, 3)).reshape(kl // span, m, width)
    terms, lines = products(chol, greens.reshape(span * wl, m, width))

    sums = jnp.sum(lines, axis=(1, 2)).reshape(span, wl, 1)
    sums = jnp.broadcast_to(sums, (span, wl, 128))
    parts, energies = spread(span, groups, terms, sums)
    own = lax.dynamic_slice(terms, (chip * wl, group * (m // groups), 0), (wl, m // groups, width))
    gradient = (own.astype(jnp.float32) + jnp.sum(parts.astype(jnp.float32), axis=0)) * gscale
    energy = lax.dynamic_index_in_dim(sums, chip, 0, keepdims=False) + jnp.sum(energies, axis=0)
    return energy[:, 0] * escale, gradient


def solution(mesh):
    span, groups = mesh.shape["walker"] // CORES, mesh.shape["chol"]
    return jax.shard_map(
        functools.partial(per_device, span, groups),
        mesh=mesh,
        in_specs=(P("chol", "walker", None), P("walker", None, None)),
        out_specs=(P("walker"), P("walker", "chol", None)),
        check_vma=False,
    )
```

```python
import functools
import math

import jax
import jax.numpy as jnp
from jax import lax
from jax.experimental import pallas as pl
from jax.experimental.pallas import tpu as pltpu
from jax.sharding import PartitionSpec as P

MESH = pl.DeviceIdType.MESH
CORES = 2
ANY = pl.BlockSpec(memory_space=pl.ANY)


def remote(src, dst, send, recv, device):
    return pltpu.make_async_remote_copy(
        src_ref=src, dst_ref=dst, send_sem=send, recv_sem=recv, device_id=device, device_id_type=MESH
    )


def greet(devices):
    barrier = pltpu.get_barrier_semaphore()
    for device in devices:
        pl.semaphore_signal(barrier, inc=1, device_id=device, device_id_type=MESH)
    pl.semaphore_wait(barrier, len(devices))


def gather_kernel(
    span, groups, chol, green, blocks, greens, own_chol, own_green,
    chol_send, chol_recv, pair_send, pair_recv, green_send, green_recv, share_send, share_recv, local,
):
    walker, group = lax.axis_index("walker"), lax.axis_index("chol")
    chip, core = walker // CORES, walker % CORES
    kept, width = blocks.shape[1], green.shape[1] // groups
    partner = (chip * CORES + 1 - core, group)
    peers = [None] + [lax.rem(chip + d, span) for d in range(1, span)]
    sources = [None] + [lax.rem(chip - d + span, span) for d in range(1, span)]
    sides = [None] + [(walker, lax.rem(group + d, groups)) for d in range(1, groups)]
    greet([partner] + [(z * CORES + core, group) for z in peers[1:]] + sides[1:])

    mine = pl.ds(pl.multiple_of(group * width, math.gcd(width, 16)), width)
    waits = []
    first, quarters = [None], [None]
    for d in range(1, span):
        target = (peers[d] * CORES + core, group)
        quarter = remote(
            green.at[:, mine, :], greens.at[chip, :, mine, :], green_send.at[d], green_recv.at[d], target
        )
        quarter.start()
        quarters.append(quarter)
    for d in range(1, span):
        target = (peers[d] * CORES + core, group)
        block = remote(
            chol.at[pl.ds(peers[d] * kept, kept)], blocks.at[walker], chol_send.at[d], chol_recv.at[d], target
        )
        block.start()
        first.append(block)
    held = chol.at[pl.ds(chip * kept, kept)]
    pair = remote(held, blocks.at[walker], pair_send.at[0], pair_recv.at[0], partner)
    pair.start()
    waits.append(pair)
    takes = [pltpu.make_async_copy(held, own_chol, local.at[0]), pltpu.make_async_copy(green, own_green, local.at[1])]
    for take in takes:
        take.start()
    for take in takes:
        take.wait()
    puts = [
        pltpu.make_async_copy(own_chol, blocks.at[walker], local.at[2]),
        pltpu.make_async_copy(own_green, greens.at[chip], local.at[3]),
    ]
    for put in puts:
        put.start()
    for d in range(1, span):
        quarters[d].wait_recv()
        piece = greens.at[sources[d], :, mine, :]
        for e in range(1, groups):
            share = remote(piece, piece, share_send.at[d, e], share_recv.at[d, e], sides[e])
            share.start()
            waits.append(share)
    for d in range(1, span):
        first[d].wait_recv()
        landed = blocks.at[sources[d] * CORES + core]
        pair = remote(landed, landed, pair_send.at[d], pair_recv.at[d], partner)
        pair.start()
        waits.append(pair)
    for put in puts:
        put.wait()
    for d in range(1, span):
        quarters[d].wait_send()
        first[d].wait_send()
    for copy in waits:
        copy.wait()


def gather(span, groups, chol, green):
    kl, mb, width = chol.shape
    wl, m, _ = green.shape
    kept = kl // span
    dma = pltpu.SemaphoreType.DMA
    return pl.pallas_call(
        functools.partial(gather_kernel, span, groups),
        out_shape=(
            jax.ShapeDtypeStruct((span * CORES, kept, mb, width), chol.dtype),
            jax.ShapeDtypeStruct((span, wl, m, width), green.dtype),
        ),
        in_specs=[ANY, ANY],
        out_specs=(ANY, ANY),
        scratch_shapes=[
            pltpu.VMEM((kept, mb, width), chol.dtype),
            pltpu.VMEM((wl, m, width), green.dtype),
            dma((span,)), dma((span,)), dma((span,)), dma((span,)), dma((span,)), dma((span,)),
            dma((span, groups)), dma((span, groups)), dma((4,)),
        ],
        compiler_params=pltpu.CompilerParams(collective_id=0, has_side_effects=True),
    )(chol, green)


def product_kernel(chol, green, terms, energy, turned, total):
    k = pl.program_id(1)
    walkers = green.shape[0]

    @pl.when(k == 0)
    def _():
        total[...] = jnp.zeros_like(total)
        energy[...] = jnp.zeros_like(energy)

    turned[...] = chol[0].T
    per = math.gcd(walkers, 4)

    def step(n, carry):
        for u in range(per):
            w = n * per + u
            tmat = jnp.dot(turned[...], green[w], preferred_element_type=jnp.float32)
            energy[w] += jnp.sum(tmat * tmat.T, axis=0, keepdims=True)
            total[w] += lax.dot_general(
                chol[0], tmat.astype(jnp.bfloat16), (((1,), (1,)), ((), ())), preferred_element_type=jnp.float32
            )
        return carry

    lax.fori_loop(0, walkers // per, step, 0)

    @pl.when(k == pl.num_programs(1) - 1)
    def _():
        terms[...] = total[...].astype(terms.dtype)


def products(chol, green):
    kept, m, width = chol.shape
    walkers = green.shape[0]
    some = math.gcd(walkers, 8)
    return pl.pallas_call(
        product_kernel,
        out_shape=(
            jax.ShapeDtypeStruct((walkers, m, width), jnp.bfloat16),
            jax.ShapeDtypeStruct((walkers, 1, width), jnp.float32),
        ),
        grid=(walkers // some, kept),
        in_specs=[
            pl.BlockSpec((1, m, width), lambda g, k: (k, 0, 0)),
            pl.BlockSpec((some, m, width), lambda g, k: (g, 0, 0)),
        ],
        out_specs=(
            pl.BlockSpec((some, m, width), lambda g, k: (g, 0, 0)),
            pl.BlockSpec((some, 1, width), lambda g, k: (g, 0, 0)),
        ),
        scratch_shapes=[pltpu.VMEM((width, m), jnp.bfloat16), pltpu.VMEM((some, m, width), jnp.float32)],
        compiler_params=pltpu.CompilerParams(
            dimension_semantics=("arbitrary", "arbitrary"), vmem_limit_bytes=60 * 2**20
        ),
    )(chol, green)


def spread_kernel(span, groups, terms, energy, parts, energies, send, recv, esend, erecv):
    walker, group = lax.axis_index("walker"), lax.axis_index("chol")
    chip, core = walker // CORES, walker % CORES
    wl, width = parts.shape[1], parts.shape[2]
    others = [(d, e) for d in range(span) for e in range(groups) if d + e > 0]
    target = {(d, e): (lax.rem(chip + d, span), lax.rem(group + e, groups)) for d, e in others}
    greet([(target[o][0] * CORES + core, target[o][1]) for o in others])
    copies = []
    for n, o in enumerate(others):
        z, q = target[o]
        device = (z * CORES + core, q)
        block = terms.at[pl.ds(z * wl, wl), pl.ds(pl.multiple_of(q * width, math.gcd(width, 16)), width), :]
        copies.append(remote(block, parts.at[n], send.at[n], recv.at[n], device))
        copies.append(remote(energy.at[z], energies.at[n], esend.at[n], erecv.at[n], device))
    for copy in copies:
        copy.start()
    for copy in copies:
        copy.wait()


def spread(span, groups, terms, energy):
    walkers, m, width = terms.shape
    count = span * groups - 1
    dma = pltpu.SemaphoreType.DMA
    return pl.pallas_call(
        functools.partial(spread_kernel, span, groups),
        out_shape=(
            jax.ShapeDtypeStruct((count, walkers // span, m // groups, width), terms.dtype),
            jax.ShapeDtypeStruct((count,) + energy.shape[1:], energy.dtype),
        ),
        in_specs=[ANY, ANY],
        out_specs=(ANY, ANY),
        scratch_shapes=[dma((count,)), dma((count,)), dma((count,)), dma((count,))],
        compiler_params=pltpu.CompilerParams(collective_id=1, has_side_effects=True),
    )(terms, energy)


LANES = 128
HALF = LANES // 2
BATCH = 4


def flip(index, bits):
    for b in range(8):
        if (bits >> b) & 1:
            step = 1 << b
            index = index + step - 2 * step * lax.rem(lax.div(index, step), 2)
    return index


def join(left, right):
    return jnp.concatenate([left, right], axis=1)


def fused_kernel(
    span, groups, escale, gscale, chol, green, out, energy,
    raw, packed, vectors, greens, turned, tmat, mixed, total, outgoing, incoming, last_out, last_in, lines, arrived,
    local, chol_send, chol_recv, pair_send, pair_recv, green_send, green_recv, share_send, share_recv,
    grad_send, grad_recv, last_send, last_recv, line_send, line_recv,
):
    walker, group = lax.axis_index("walker"), lax.axis_index("chol")
    chip, core = lax.div(walker, CORES), lax.rem(walker, CORES)
    kept, mb = raw.shape[1], raw.shape[2]
    m = total.shape[1]
    chunks = kept // BATCH
    quarter = m // groups
    part = quarter // 2
    cell = 3 * LANES
    bits = [1 << b for b in range(groups.bit_length() - 1)]
    orders = [bits, bits[::-1]]
    partner = (chip * CORES + 1 - core, group)

    def device(r, e):
        return (flip(chip, r) * CORES + core, flip(group, e))

    slots = [flip(chip, r) for r in range(span)]
    turns = list(range(span - 1, 0, -1))
    others = [(r, 0) for r in range(1, span)] + [(0, e) for e in range(1, groups)]
    barrier = pltpu.get_barrier_semaphore()
    for peer in [partner] + [device(r, e) for r, e in others]:
        pl.semaphore_signal(barrier, inc=1, device_id=peer, device_id_type=MESH)

    loads = [
        pltpu.make_async_copy(chol.at[pl.ds(flip(chip, r) * kept, kept)], raw.at[r], local.at[r]) for r in range(span)
    ]
    greens_in = []
    for w in range(CORES):
        for rows, tile, at in ((slice(0, LANES), w, 0), (slice(LANES, LANES + HALF), 2, w * HALF)):
            greens_in.append(
                pltpu.make_async_copy(
                    green.at[w, rows], turned.at[3 * chip + tile, at : at + rows.stop - rows.start], local.at[span + len(greens_in)]
                )
            )
    for copy in greens_in:
        copy.start()
    for r in reversed(range(span)):
        loads[r].start()

    def pack(r, ch):
        pieces = []
        for p in range(BATCH // 2):
            a = raw[r, ch * BATCH + 2 * p]
            b = raw[r, ch * BATCH + 2 * p + 1]
            pieces += [a[:, :LANES], b[:, :LANES], join(a[:, LANES:], b[:, LANES:])]
        return pieces

    def pack_chunk(ch):
        for r in range(span):
            for n, piece in enumerate(pack(r, ch)):
                if r == 0:
                    vectors[ch, walker, :, n * LANES : (n + 1) * LANES] = piece
                else:
                    packed[r, ch, :, n * LANES : (n + 1) * LANES] = piece

    def chol_copy(ch, r):
        return remote(packed.at[r, ch], vectors.at[ch, walker], chol_send.at[ch, r], chol_recv.at[ch, r], device(r, 0))

    def pair_copy(ch, r):
        block = vectors.at[ch, flip(chip, r) * CORES + core]
        return remote(block, block, pair_send.at[ch, r], pair_recv.at[ch, r], partner)

    def green_piece(r, e):
        size = LANES // groups
        rows = pl.ds(pl.multiple_of(flip(group, e) * size, 16), size)
        return turned.at[pl.ds(3 * flip(chip, r), 3), rows, :]

    def green_copy(r, bit):
        n = r | bit
        return remote(green_piece(r, 0), green_piece(r, 0), green_send.at[n], green_recv.at[n], device(bit, 0))

    def share_copy(r, e):
        return remote(green_piece(r, 0), green_piece(r, 0), share_send.at[r, e], share_recv.at[r, e], device(0, e))

    for copy in greens_in:
        copy.wait()
    pl.semaphore_wait(barrier, len(others) + 1)

    highs = [1 << b for b in reversed(range(span.bit_length() - 1))]
    for bit in highs:
        green_copy(0, bit).start()
    for r in reversed(range(span)):
        loads[r].wait()
    pack_chunk(0)
    for r in turns:
        chol_copy(0, r).start()
    pair_copy(0, 0).start()

    def pack_rest(ch, carry):
        pack_chunk(ch)
        return carry

    lax.fori_loop(1, chunks, pack_rest, 0)
    total[...] = jnp.zeros_like(total)

    for at, bit in enumerate(highs):
        done = [r for r in range(span) if r % (2 * bit) == 0]
        for r in done:
            n = r | bit
            green_copy(r, bit).wait_recv()
            for low in highs[at + 1 :]:
                green_copy(n, low).start()
            for e in range(1, groups):
                share_copy(n, e).start()

    def send_rest(ch, carry):
        for r in turns:
            chol_copy(ch, r).start()
        pair_copy(ch, 0).start()
        return carry

    lax.fori_loop(1, chunks, send_rest, 0)

    for r in range(1, span):
        for e in range(1, groups):
            share_copy(r, e).wait_recv()

    def turn(n, carry):
        greens[n] = turned[n].T
        return carry

    lax.fori_loop(0, 3 * span, turn, 0)

    def compute(ch, s):
        left = turned[pl.ds(3 * s, 3)].reshape(cell, m)
        for n in range(3):
            cut = slice(2 * n * LANES, 2 * (n + 1) * LANES)
            right = vectors[ch, :, :, cut].reshape(m, 2 * LANES)
            tmat[:, cut] = jnp.dot(left, right, preferred_element_type=jnp.float32).astype(jnp.bfloat16)
        for k in range(2):
            for at, size in ((0, LANES), (2 * LANES, HALF)):
                source = [slice(at + size * b, at + size * (b + 1)) for b in range(2)]
                target = [slice(k * cell + at + size * a, k * cell + at + size * (a + 1)) for a in range(2)]
                for a in range(2):
                    for b in range(2):
                        mixed[target[a], b * LANES : (b + 1) * LANES] = tmat[
                            source[b], k * cell + a * LANES : k * cell + (a + 1) * LANES
                        ]
                ends = [tmat[source[b], k * cell + 2 * LANES : (k + 1) * cell] for b in range(2)]
                for a in range(2):
                    half = slice(a * HALF, (a + 1) * HALF)
                    mixed[target[a], 2 * LANES :] = join(ends[0][:, half], ends[1][:, half])
        whole = vectors[ch].reshape(m, 2 * cell)
        for first, size in ((0, 2), (2, 1)):
            cut = slice(first * LANES, (first + size) * LANES)
            sums = jnp.dot(whole, mixed[:, cut], preferred_element_type=jnp.float32)
            for t in range(size):
                total[3 * s + first + t] += sums[:, t * LANES : (t + 1) * LANES]

    def rows_of(e, colour):
        return pl.ds(pl.multiple_of(flip(group, e) * quarter + colour * part, 16), part)

    def held(r, e, colour):
        return total.at[pl.ds(3 * r, 3), rows_of(e, colour), :]

    def grad_copy(s, colour, e, bit):
        return remote(
            outgoing.at[s, colour, e], incoming.at[s, colour, e], grad_send.at[s, colour, e], grad_recv.at[s, colour, e],
            device(0, bit),
        )

    def ready(order, at):
        past = sum(order[:at])
        sent = [e for e in range(groups) if (e & order[at]) and not (e & past)]
        return sorted(sent, key=lambda e: e == order[at])

    def convert(s):
        for colour, order in enumerate(orders):
            for e in ready(order, 0):
                outgoing[s, colour, e] = held(s, e, colour)[...].astype(jnp.bfloat16)

    def send_first(s, n):
        for colour, order in enumerate(orders):
            grad_copy(s, colour, ready(order, 0)[n], order[0]).start()

    low = lax.broadcasted_iota(jnp.int32, (8, LANES), 1) < HALF

    def weigh(s):
        def rows(n, sums):
            at = pl.ds(pl.multiple_of(n * 64, 64), 64)
            new = []
            for t in range(3):
                product = greens[3 * s + t, at, :].astype(jnp.float32) * total[3 * s + t, at, :]
                new.append(sums[t] + jnp.sum(product.reshape(8, 8, LANES), axis=0))
            return tuple(new)

        zero = jnp.zeros((8, LANES), jnp.float32)
        sums = lax.fori_loop(0, m // 64, rows, (zero, zero, zero))
        lines[s, :1] = jnp.sum(sums[0] + jnp.where(low, sums[2], 0.0), axis=0, keepdims=True)
        lines[s, 1:] = jnp.sum(sums[1] + jnp.where(low, 0.0, sums[2]), axis=0, keepdims=True)

    def chunk_step(ch, carry):
        for r in turns:
            chol_copy(ch, r).wait_recv()
            pair_copy(ch, r).start()
        for r in range(span):
            pair_copy(ch, r).wait_recv()

        for r in reversed(range(span)):
            compute(ch, slots[r])

            @pl.when(ch == chunks - 1)
            def _():
                convert(slots[r])
                if r > 1:
                    for n in range(groups // 2):
                        send_first(slots[r], n)
                weigh(slots[r])

        return carry

    lax.fori_loop(0, chunks, chunk_step, 0)

    def line_copy(n):
        r, e = others[n]
        source = lines.at[slots[r]] if e == 0 else lines.at[span]
        return remote(source, arrived.at[n], line_send.at[n], line_recv.at[n], device(r, e))

    def take(r, at, n):
        s = slots[r]
        for colour, order in enumerate(orders):
            e = ready(order, at)[n]
            grad_copy(s, colour, e, order[at]).wait_recv()
            mine = e ^ order[at]
            piece = held(s, mine, colour)
            value = piece[...] + incoming[s, colour, e].astype(jnp.float32)
            if at + 1 < len(order) and mine & order[at + 1]:
                outgoing[s, colour, mine] = value.astype(jnp.bfloat16)
                grad_copy(s, colour, mine, order[at + 1]).start()
            else:
                piece[...] = value

    def last_copy(r):
        return remote(last_out.at[r], last_in.at[r], last_send.at[r], last_recv.at[r], device(r, 0))

    mine = pl.ds(pl.multiple_of(group * quarter, 16), quarter)

    def settle(r):
        take(r, 1, 0)
        if r > 0:
            last_out[r] = total[pl.ds(3 * slots[r], 3), mine, :].astype(jnp.bfloat16)
            last_copy(r).start()

    take(3, 0, 0)
    take(3, 0, 1)
    take(2, 0, 0)
    send_first(slots[1], 0)
    send_first(slots[1], 1)
    for n in range(span - 1):
        line_copy(n).start()
    take(2, 0, 1)
    settle(3)
    send_first(slots[0], 0)
    settle(2)
    sums = lines[chip]
    for n in range(span - 1):
        line_copy(n).wait_recv()
        sums = sums + arrived[n]
    lines[span] = sums
    take(1, 0, 0)
    send_first(slots[0], 1)
    take(1, 0, 1)
    for n in range(span - 1, len(others)):
        line_copy(n).start()
    take(0, 0, 0)
    settle(1)
    take(0, 0, 1)
    settle(0)

    for r in range(1, span):
        last_copy(r).wait_recv()
    final = [total[3 * chip + t, mine, :] for t in range(3)]
    for r in range(1, span):
        final = [final[t] + last_in[r, t].astype(jnp.float32) for t in range(3)]
    final = [x * gscale for x in final]
    out[0, :, :LANES] = final[0]
    out[1, :, :LANES] = final[1]
    out[0, :, LANES:] = final[2][:, :HALF]
    out[1, :, LANES:] = final[2][:, HALF:]

    sums = lines[span]
    for n in range(span - 1, len(others)):
        line_copy(n).wait_recv()
        sums = sums + arrived[n]
    sums = jnp.sum(sums, axis=1, keepdims=True) * escale
    energy[...] = join(sums[:1], sums[1:])

    for bit in highs:
        for r in range(span):
            if r % (2 * bit) == 0:
                green_copy(r, bit).wait_send()
    for r in range(1, span):
        for e in range(1, groups):
            share_copy(r, e).wait_send()

    def drain(ch, carry):
        for r in range(1, span):
            chol_copy(ch, r).wait_send()
        for r in range(span):
            pair_copy(ch, r).wait_send()
        return carry

    lax.fori_loop(0, chunks, drain, 0)
    for s in range(span):
        for colour, order in enumerate(orders):
            for at, bit in enumerate(order):
                for e in range(groups):
                    if (e & bit) and not (e & sum(order[:at])):
                        grad_copy(s, colour, e, bit).wait_send()
    for r in range(1, span):
        last_copy(r).wait_send()
    for n in range(len(others)):
        line_copy(n).wait_send()


def fused(span, groups, escale, gscale, chol, green):
    kl, mb, width = chol.shape
    wl, m, _ = green.shape
    kept = kl // span
    chunks = kept // BATCH
    quarter = m // groups
    count = span + groups - 2
    cell = 3 * LANES
    dma = pltpu.SemaphoreType.DMA
    half, full = jnp.bfloat16, jnp.float32
    return pl.pallas_call(
        functools.partial(fused_kernel, span, groups, escale, gscale),
        out_shape=(
            pltpu.VMEM((wl, quarter, width), full),
            pltpu.VMEM((1, wl), full),
        ),
        in_specs=[ANY, ANY],
        out_specs=(pl.BlockSpec(memory_space=pltpu.VMEM), pl.BlockSpec(memory_space=pltpu.VMEM)),
        scratch_shapes=[
            pltpu.VMEM((span, kept, mb, width), half),
            pltpu.VMEM((span, chunks, mb, 2 * cell), half),
            pltpu.VMEM((chunks, span * CORES, mb, 2 * cell), half),
            pltpu.VMEM((3 * span, m, LANES), half),
            pltpu.VMEM((3 * span, LANES, m), half),
            pltpu.VMEM((cell, 2 * cell), half),
            pltpu.VMEM((2 * cell, cell), half),
            pltpu.VMEM((3 * span, m, LANES), full),
            pltpu.VMEM((span, 2, groups, 3, quarter // 2, LANES), half),
            pltpu.VMEM((span, 2, groups, 3, quarter // 2, LANES), half),
            pltpu.VMEM((span, 3, quarter, LANES), half),
            pltpu.VMEM((span, 3, quarter, LANES), half),
            pltpu.VMEM((span + 1, wl, LANES), full),
            pltpu.VMEM((count, wl, LANES), full),
            dma((span + 2 * wl,)),
            dma((chunks, span)), dma((chunks, span)), dma((chunks, span)), dma((chunks, span)),
            dma((span,)), dma((span,)), dma((span, groups)), dma((span, groups)),
            dma((span, 2, groups)), dma((span, 2, groups)), dma((span,)), dma((span,)), dma((count,)), dma((count,)),
        ],
        compiler_params=pltpu.CompilerParams(collective_id=2, has_side_effects=True, vmem_limit_bytes=60 * 2**20),
    )(chol, jnp.swapaxes(green, 1, 2))


def fits(span, groups, chol, green):
    kl, mb, width = chol.shape
    wl, m, _ = green.shape
    powers = span & (span - 1) == 0 and groups & (groups - 1) == 0
    tiles = width == LANES + HALF and wl == 2 and mb % 16 == 0 and m % 64 == 0 and m % (groups * 32) == 0
    return powers and tiles and span == 4 and groups == 4 and kl % (span * BATCH) == 0 and span * m * width <= 2**21


def per_device(span, groups, chol_vectors, green):
    kl, mb, width = chol_vectors.shape
    wl, m, _ = green.shape
    nchol = kl * groups
    escale = 1.0 / (nchol * width)
    gscale = 1.0 / nchol**0.5
    chip, group = lax.axis_index("walker") // CORES, lax.axis_index("chol")

    if fits(span, groups, chol_vectors, green):
        gradient, energy = fused(span, groups, escale, gscale, chol_vectors, green)
        return energy[0], gradient

    blocks, greens = gather(span, groups, chol_vectors, green)
    chol = jnp.transpose(blocks, (1, 0, 2, 3)).reshape(kl // span, m, width)
    terms, lines = products(chol, greens.reshape(span * wl, m, width))

    sums = jnp.sum(lines, axis=(1, 2)).reshape(span, wl, 1)
    sums = jnp.broadcast_to(sums, (span, wl, 128))
    parts, energies = spread(span, groups, terms, sums)
    own = lax.dynamic_slice(terms, (chip * wl, group * (m // groups), 0), (wl, m // groups, width))
    gradient = (own.astype(jnp.float32) + jnp.sum(parts.astype(jnp.float32), axis=0)) * gscale
    energy = lax.dynamic_index_in_dim(sums, chip, 0, keepdims=False) + jnp.sum(energies, axis=0)
    return energy[:, 0] * escale, gradient


def solution(mesh):
    span, groups = mesh.shape["walker"] // CORES, mesh.shape["chol"]
    return jax.shard_map(
        functools.partial(per_device, span, groups),
        mesh=mesh,
        in_specs=(P("chol", "walker", None), P("walker", None, None)),
        out_specs=(P("walker"), P("walker", "chol", None)),
        check_vma=False,
    )
```

```python
import functools
import math

import jax
import jax.numpy as jnp
from jax import lax
from jax.experimental import pallas as pl
from jax.experimental.pallas import tpu as pltpu
from jax.sharding import PartitionSpec as P

MESH = pl.DeviceIdType.MESH
CORES = 2
ANY = pl.BlockSpec(memory_space=pl.ANY)


def remote(src, dst, send, recv, device):
    return pltpu.make_async_remote_copy(
        src_ref=src, dst_ref=dst, send_sem=send, recv_sem=recv, device_id=device, device_id_type=MESH
    )


def greet(devices):
    barrier = pltpu.get_barrier_semaphore()
    for device in devices:
        pl.semaphore_signal(barrier, inc=1, device_id=device, device_id_type=MESH)
    pl.semaphore_wait(barrier, len(devices))


def gather_kernel(
    span, groups, chol, green, blocks, greens, own_chol, own_green,
    chol_send, chol_recv, pair_send, pair_recv, green_send, green_recv, share_send, share_recv, local,
):
    walker, group = lax.axis_index("walker"), lax.axis_index("chol")
    chip, core = walker // CORES, walker % CORES
    kept, width = blocks.shape[1], green.shape[1] // groups
    partner = (chip * CORES + 1 - core, group)
    peers = [None] + [lax.rem(chip + d, span) for d in range(1, span)]
    sources = [None] + [lax.rem(chip - d + span, span) for d in range(1, span)]
    sides = [None] + [(walker, lax.rem(group + d, groups)) for d in range(1, groups)]
    greet([partner] + [(z * CORES + core, group) for z in peers[1:]] + sides[1:])

    mine = pl.ds(pl.multiple_of(group * width, math.gcd(width, 16)), width)
    waits = []
    first, quarters = [None], [None]
    for d in range(1, span):
        target = (peers[d] * CORES + core, group)
        quarter = remote(
            green.at[:, mine, :], greens.at[chip, :, mine, :], green_send.at[d], green_recv.at[d], target
        )
        quarter.start()
        quarters.append(quarter)
    for d in range(1, span):
        target = (peers[d] * CORES + core, group)
        block = remote(
            chol.at[pl.ds(peers[d] * kept, kept)], blocks.at[walker], chol_send.at[d], chol_recv.at[d], target
        )
        block.start()
        first.append(block)
    held = chol.at[pl.ds(chip * kept, kept)]
    pair = remote(held, blocks.at[walker], pair_send.at[0], pair_recv.at[0], partner)
    pair.start()
    waits.append(pair)
    takes = [pltpu.make_async_copy(held, own_chol, local.at[0]), pltpu.make_async_copy(green, own_green, local.at[1])]
    for take in takes:
        take.start()
    for take in takes:
        take.wait()
    puts = [
        pltpu.make_async_copy(own_chol, blocks.at[walker], local.at[2]),
        pltpu.make_async_copy(own_green, greens.at[chip], local.at[3]),
    ]
    for put in puts:
        put.start()
    for d in range(1, span):
        quarters[d].wait_recv()
        piece = greens.at[sources[d], :, mine, :]
        for e in range(1, groups):
            share = remote(piece, piece, share_send.at[d, e], share_recv.at[d, e], sides[e])
            share.start()
            waits.append(share)
    for d in range(1, span):
        first[d].wait_recv()
        landed = blocks.at[sources[d] * CORES + core]
        pair = remote(landed, landed, pair_send.at[d], pair_recv.at[d], partner)
        pair.start()
        waits.append(pair)
    for put in puts:
        put.wait()
    for d in range(1, span):
        quarters[d].wait_send()
        first[d].wait_send()
    for copy in waits:
        copy.wait()


def gather(span, groups, chol, green):
    kl, mb, width = chol.shape
    wl, m, _ = green.shape
    kept = kl // span
    dma = pltpu.SemaphoreType.DMA
    return pl.pallas_call(
        functools.partial(gather_kernel, span, groups),
        out_shape=(
            jax.ShapeDtypeStruct((span * CORES, kept, mb, width), chol.dtype),
            jax.ShapeDtypeStruct((span, wl, m, width), green.dtype),
        ),
        in_specs=[ANY, ANY],
        out_specs=(ANY, ANY),
        scratch_shapes=[
            pltpu.VMEM((kept, mb, width), chol.dtype),
            pltpu.VMEM((wl, m, width), green.dtype),
            dma((span,)), dma((span,)), dma((span,)), dma((span,)), dma((span,)), dma((span,)),
            dma((span, groups)), dma((span, groups)), dma((4,)),
        ],
        compiler_params=pltpu.CompilerParams(collective_id=0, has_side_effects=True),
    )(chol, green)


def product_kernel(chol, green, terms, energy, turned, total):
    k = pl.program_id(1)
    walkers = green.shape[0]

    @pl.when(k == 0)
    def _():
        total[...] = jnp.zeros_like(total)
        energy[...] = jnp.zeros_like(energy)

    turned[...] = chol[0].T
    per = math.gcd(walkers, 4)

    def step(n, carry):
        for u in range(per):
            w = n * per + u
            tmat = jnp.dot(turned[...], green[w], preferred_element_type=jnp.float32)
            energy[w] += jnp.sum(tmat * tmat.T, axis=0, keepdims=True)
            total[w] += lax.dot_general(
                chol[0], tmat.astype(jnp.bfloat16), (((1,), (1,)), ((), ())), preferred_element_type=jnp.float32
            )
        return carry

    lax.fori_loop(0, walkers // per, step, 0)

    @pl.when(k == pl.num_programs(1) - 1)
    def _():
        terms[...] = total[...].astype(terms.dtype)


def products(chol, green):
    kept, m, width = chol.shape
    walkers = green.shape[0]
    some = math.gcd(walkers, 8)
    return pl.pallas_call(
        product_kernel,
        out_shape=(
            jax.ShapeDtypeStruct((walkers, m, width), jnp.bfloat16),
            jax.ShapeDtypeStruct((walkers, 1, width), jnp.float32),
        ),
        grid=(walkers // some, kept),
        in_specs=[
            pl.BlockSpec((1, m, width), lambda g, k: (k, 0, 0)),
            pl.BlockSpec((some, m, width), lambda g, k: (g, 0, 0)),
        ],
        out_specs=(
            pl.BlockSpec((some, m, width), lambda g, k: (g, 0, 0)),
            pl.BlockSpec((some, 1, width), lambda g, k: (g, 0, 0)),
        ),
        scratch_shapes=[pltpu.VMEM((width, m), jnp.bfloat16), pltpu.VMEM((some, m, width), jnp.float32)],
        compiler_params=pltpu.CompilerParams(
            dimension_semantics=("arbitrary", "arbitrary"), vmem_limit_bytes=60 * 2**20
        ),
    )(chol, green)


def spread_kernel(span, groups, terms, energy, parts, energies, send, recv, esend, erecv):
    walker, group = lax.axis_index("walker"), lax.axis_index("chol")
    chip, core = walker // CORES, walker % CORES
    wl, width = parts.shape[1], parts.shape[2]
    others = [(d, e) for d in range(span) for e in range(groups) if d + e > 0]
    target = {(d, e): (lax.rem(chip + d, span), lax.rem(group + e, groups)) for d, e in others}
    greet([(target[o][0] * CORES + core, target[o][1]) for o in others])
    copies = []
    for n, o in enumerate(others):
        z, q = target[o]
        device = (z * CORES + core, q)
        block = terms.at[pl.ds(z * wl, wl), pl.ds(pl.multiple_of(q * width, math.gcd(width, 16)), width), :]
        copies.append(remote(block, parts.at[n], send.at[n], recv.at[n], device))
        copies.append(remote(energy.at[z], energies.at[n], esend.at[n], erecv.at[n], device))
    for copy in copies:
        copy.start()
    for copy in copies:
        copy.wait()


def spread(span, groups, terms, energy):
    walkers, m, width = terms.shape
    count = span * groups - 1
    dma = pltpu.SemaphoreType.DMA
    return pl.pallas_call(
        functools.partial(spread_kernel, span, groups),
        out_shape=(
            jax.ShapeDtypeStruct((count, walkers // span, m // groups, width), terms.dtype),
            jax.ShapeDtypeStruct((count,) + energy.shape[1:], energy.dtype),
        ),
        in_specs=[ANY, ANY],
        out_specs=(ANY, ANY),
        scratch_shapes=[dma((count,)), dma((count,)), dma((count,)), dma((count,))],
        compiler_params=pltpu.CompilerParams(collective_id=1, has_side_effects=True),
    )(terms, energy)


LANES = 128
HALF = LANES // 2
BATCH = 4


def flip(index, bits):
    for b in range(8):
        if (bits >> b) & 1:
            step = 1 << b
            index = index + step - 2 * step * lax.rem(lax.div(index, step), 2)
    return index


def join(left, right):
    return jnp.concatenate([left, right], axis=1)


def fused_kernel(
    span, groups, escale, gscale, chol, green, out, energy,
    raw, packed, vectors, greens, turned, tmat, mixed, total, outgoing, incoming, last_out, last_in, near_out, near_in, lines, arrived,
    local, chol_send, chol_recv, pair_send, pair_recv, green_send, green_recv, share_send, share_recv,
    grad_send, grad_recv, near_send, near_recv, last_send, last_recv, line_send, line_recv,
):
    walker, group = lax.axis_index("walker"), lax.axis_index("chol")
    chip, core = lax.div(walker, CORES), lax.rem(walker, CORES)
    kept, mb = raw.shape[1], raw.shape[2]
    m = total.shape[1]
    chunks = kept // BATCH
    quarter = m // groups
    part = quarter // 2
    cell = 3 * LANES
    sides = [flip(group, e) for e in range(groups)]
    near, plain = core, 1 - core
    partner = (chip * CORES + 1 - core, group)

    def device(r, e):
        return (flip(chip, r) * CORES + core, flip(group, e))

    slots = [flip(chip, r) for r in range(span)]
    turns = list(range(span - 1, 0, -1))
    others = [(r, 0) for r in range(1, span)] + [(0, e) for e in range(1, groups)]
    barrier = pltpu.get_barrier_semaphore()
    for peer in [partner] + [device(r, e) for r, e in others]:
        pl.semaphore_signal(barrier, inc=1, device_id=peer, device_id_type=MESH)

    loads = [
        pltpu.make_async_copy(chol.at[pl.ds(flip(chip, r) * kept, kept)], raw.at[r], local.at[r]) for r in range(span)
    ]
    greens_in = []
    for w in range(CORES):
        for rows, tile, at in ((slice(0, LANES), w, 0), (slice(LANES, LANES + HALF), 2, w * HALF)):
            greens_in.append(
                pltpu.make_async_copy(
                    green.at[w, rows], turned.at[3 * chip + tile, at : at + rows.stop - rows.start], local.at[span + len(greens_in)]
                )
            )
    for copy in greens_in:
        copy.start()
    for r in reversed(range(span)):
        loads[r].start()

    def pack(r, ch):
        pieces = []
        for p in range(BATCH // 2):
            a = raw[r, ch * BATCH + 2 * p]
            b = raw[r, ch * BATCH + 2 * p + 1]
            pieces += [a[:, :LANES], b[:, :LANES], join(a[:, LANES:], b[:, LANES:])]
        return pieces

    def pack_chunk(ch):
        for r in range(span):
            for n, piece in enumerate(pack(r, ch)):
                if r == 0:
                    vectors[ch, walker, :, n * LANES : (n + 1) * LANES] = piece
                else:
                    packed[r, ch, :, n * LANES : (n + 1) * LANES] = piece

    def chol_copy(ch, r):
        return remote(packed.at[r, ch], vectors.at[ch, walker], chol_send.at[ch, r], chol_recv.at[ch, r], device(r, 0))

    def pair_copy(ch, r):
        block = vectors.at[ch, flip(chip, r) * CORES + core]
        return remote(block, block, pair_send.at[ch, r], pair_recv.at[ch, r], partner)

    def green_piece(r, e):
        size = LANES // groups
        rows = pl.ds(pl.multiple_of(flip(group, e) * size, 16), size)
        return turned.at[pl.ds(3 * flip(chip, r), 3), rows, :]

    def green_copy(r, bit):
        n = r | bit
        return remote(green_piece(r, 0), green_piece(r, 0), green_send.at[n], green_recv.at[n], device(bit, 0))

    def share_copy(r, e):
        return remote(green_piece(r, 0), green_piece(r, 0), share_send.at[r, e], share_recv.at[r, e], device(0, e))

    for copy in greens_in:
        copy.wait()
    pl.semaphore_wait(barrier, len(others) + 1)

    highs = [1 << b for b in reversed(range(span.bit_length() - 1))]
    for bit in highs:
        green_copy(0, bit).start()
    for r in reversed(range(span)):
        loads[r].wait()
    pack_chunk(0)
    for r in turns:
        chol_copy(0, r).start()
    pair_copy(0, 0).start()

    def pack_rest(ch, carry):
        pack_chunk(ch)
        return carry

    lax.fori_loop(1, chunks, pack_rest, 0)
    total[...] = jnp.zeros_like(total)

    for at, bit in enumerate(highs):
        done = [r for r in range(span) if r % (2 * bit) == 0]
        for r in done:
            n = r | bit
            green_copy(r, bit).wait_recv()
            for low in highs[at + 1 :]:
                green_copy(n, low).start()
            for e in range(1, groups):
                share_copy(n, e).start()

    def send_rest(ch, carry):
        for r in turns:
            chol_copy(ch, r).start()
        pair_copy(ch, 0).start()
        return carry

    lax.fori_loop(1, chunks, send_rest, 0)

    for r in range(1, span):
        for e in range(1, groups):
            share_copy(r, e).wait_recv()

    def turn(n, carry):
        greens[n] = turned[n].T
        return carry

    lax.fori_loop(0, 3 * span, turn, 0)

    def compute(ch, s):
        left = turned[pl.ds(3 * s, 3)].reshape(cell, m)
        for n in range(3):
            cut = slice(2 * n * LANES, 2 * (n + 1) * LANES)
            right = vectors[ch, :, :, cut].reshape(m, 2 * LANES)
            tmat[:, cut] = jnp.dot(left, right, preferred_element_type=jnp.float32).astype(jnp.bfloat16)
        for k in range(2):
            for at, size in ((0, LANES), (2 * LANES, HALF)):
                source = [slice(at + size * b, at + size * (b + 1)) for b in range(2)]
                target = [slice(k * cell + at + size * a, k * cell + at + size * (a + 1)) for a in range(2)]
                for a in range(2):
                    for b in range(2):
                        mixed[target[a], b * LANES : (b + 1) * LANES] = tmat[
                            source[b], k * cell + a * LANES : k * cell + (a + 1) * LANES
                        ]
                ends = [tmat[source[b], k * cell + 2 * LANES : (k + 1) * cell] for b in range(2)]
                for a in range(2):
                    half = slice(a * HALF, (a + 1) * HALF)
                    mixed[target[a], 2 * LANES :] = join(ends[0][:, half], ends[1][:, half])
        whole = vectors[ch].reshape(m, 2 * cell)
        for first, size in ((0, 2), (2, 1)):
            cut = slice(first * LANES, (first + size) * LANES)
            sums = jnp.dot(whole, mixed[:, cut], preferred_element_type=jnp.float32)
            for t in range(size):
                total[3 * s + first + t] += sums[:, t * LANES : (t + 1) * LANES]

    def routes(colour):
        first = sides[1] + colour * (sides[2] - sides[1])
        return first, sides[1] + sides[2] - first, sides[3]

    def held(s, block, colour):
        return total.at[pl.ds(3 * s, 3), pl.ds(pl.multiple_of(block * quarter + colour * part, 16), part), :]

    def grad_copy(s, colour, kind):
        first, second, _ = routes(colour)
        return remote(
            outgoing.at[s, colour, kind], incoming.at[s, colour, kind],
            grad_send.at[s, colour, kind], grad_recv.at[s, colour, kind], (walker, second if kind == 2 else first),
        )

    def convert(s, colour):
        first, _, both = routes(colour)
        outgoing[s, colour, 0] = held(s, both, colour)[...].astype(jnp.bfloat16)
        outgoing[s, colour, 1] = held(s, first, colour)[...].astype(jnp.bfloat16)

    def near_copy():
        return remote(near_out, near_in, near_send.at[0], near_recv.at[0], device(1, 0))

    low = lax.broadcasted_iota(jnp.int32, (8, LANES), 1) < HALF

    def weigh(s):
        def rows(n, sums):
            at = pl.ds(pl.multiple_of(n * 64, 64), 64)
            new = []
            for t in range(3):
                product = greens[3 * s + t, at, :].astype(jnp.float32) * total[3 * s + t, at, :]
                new.append(sums[t] + jnp.sum(product.reshape(8, 8, LANES), axis=0))
            return tuple(new)

        zero = jnp.zeros((8, LANES), jnp.float32)
        sums = lax.fori_loop(0, m // 64, rows, (zero, zero, zero))
        lines[s, :1] = jnp.sum(sums[0] + jnp.where(low, sums[2], 0.0), axis=0, keepdims=True)
        lines[s, 1:] = jnp.sum(sums[1] + jnp.where(low, 0.0, sums[2]), axis=0, keepdims=True)

    def chunk_step(ch, carry):
        for r in reversed(turns):
            chol_copy(ch, r).wait_recv()
            pair_copy(ch, r).start()
        for r in range(span):
            pair_copy(ch, r).wait_recv()

        for r in (3, 1, 2, 0):
            compute(ch, slots[r])

            @pl.when(ch == chunks - 1)
            def _():
                if r > 1:
                    convert(slots[r], 0)
                    convert(slots[r], 1)
                    for kind in range(2):
                        grad_copy(slots[r], 0, kind).start()
                        grad_copy(slots[r], 1, kind).start()
                else:
                    convert(slots[r], plain)
                if r == 1:
                    for block in range(groups):
                        near_out[block] = held(slots[1], block, near)[...].astype(jnp.bfloat16)
                    near_copy().start()
                weigh(slots[r])

        return carry

    lax.fori_loop(0, chunks, chunk_step, 0)

    def line_copy(n):
        r, e = others[n]
        source = lines.at[slots[r]] if e == 0 else lines.at[span]
        return remote(source, arrived.at[n], line_send.at[n], line_recv.at[n], device(r, e))

    def take(r, kind, colours):
        s = slots[r]
        for colour in colours:
            grad_copy(s, colour, kind).wait_recv()
            piece = held(s, group if kind else routes(colour)[1], colour)
            value = piece[...] + incoming[s, colour, kind].astype(jnp.float32)
            if kind == 0:
                outgoing[s, colour, 2] = value.astype(jnp.bfloat16)
                grad_copy(s, colour, 2).start()
            else:
                piece[...] = value

    def send_first(r, colour):
        for kind in range(2):
            grad_copy(slots[r], colour, kind).start()

    mine = pl.ds(pl.multiple_of(group * quarter, 16), quarter)

    def last_copy(r, colour):
        return remote(
            last_out.at[r, colour], last_in.at[r, colour], last_send.at[r, colour], last_recv.at[r, colour], device(r, 0)
        )

    def settle(r, colours):
        for colour in colours:
            take(r, 2, (colour,))
            last_out[r, colour] = held(slots[r], group, colour)[...].astype(jnp.bfloat16)
            last_copy(r, colour).start()

    take(3, 0, (0, 1))
    take(3, 1, (0, 1))
    take(2, 0, (0, 1))
    send_first(1, plain)
    for n in range(span - 1):
        line_copy(n).start()
    take(2, 1, (0, 1))
    settle(3, (0, 1))
    send_first(0, plain)
    settle(2, (0, 1))
    sums = lines[chip]
    for n in range(span - 1):
        line_copy(n).wait_recv()
        sums = sums + arrived[n]
    lines[span] = sums
    take(1, 0, (plain,))
    near_copy().wait_recv()
    for block in range(groups):
        piece = held(chip, block, near)
        piece[...] = piece[...] + near_in[block].astype(jnp.float32)
    convert(chip, near)
    send_first(0, near)
    take(1, 1, (plain,))
    for n in range(span - 1, len(others)):
        line_copy(n).start()
    take(0, 0, (plain,))
    take(0, 1, (plain,))
    settle(1, (plain,))
    take(0, 0, (near,))
    take(0, 1, (near,))
    take(0, 2, (plain, near))

    for r in range(span - 1, 0, -1):
        for colour in (plain,) if r == 1 else (0, 1):
            last_copy(r, colour).wait_recv()
            piece = held(chip, group, colour)
            piece[...] = piece[...] + last_in[r, colour].astype(jnp.float32)
    final = [total[3 * chip + t, mine, :] for t in range(3)]
    final = [x * gscale for x in final]
    out[0, :, :LANES] = final[0]
    out[1, :, :LANES] = final[1]
    out[0, :, LANES:] = final[2][:, :HALF]
    out[1, :, LANES:] = final[2][:, HALF:]

    sums = lines[span]
    for n in range(span - 1, len(others)):
        line_copy(n).wait_recv()
        sums = sums + arrived[n]
    sums = jnp.sum(sums, axis=1, keepdims=True) * escale
    energy[...] = join(sums[:1], sums[1:])

    for bit in highs:
        for r in range(span):
            if r % (2 * bit) == 0:
                green_copy(r, bit).wait_send()
    for r in range(1, span):
        for e in range(1, groups):
            share_copy(r, e).wait_send()

    def drain(ch, carry):
        for r in range(1, span):
            chol_copy(ch, r).wait_send()
        for r in range(span):
            pair_copy(ch, r).wait_send()
        return carry

    lax.fori_loop(0, chunks, drain, 0)
    for r in range(span):
        for colour in (plain,) if r == 1 else (0, 1):
            for kind in range(3):
                grad_copy(slots[r], colour, kind).wait_send()
    near_copy().wait_send()
    for r in range(1, span):
        for colour in (plain,) if r == 1 else (0, 1):
            last_copy(r, colour).wait_send()
    for n in range(len(others)):
        line_copy(n).wait_send()


def fused(span, groups, escale, gscale, chol, green):
    kl, mb, width = chol.shape
    wl, m, _ = green.shape
    kept = kl // span
    chunks = kept // BATCH
    quarter = m // groups
    count = span + groups - 2
    cell = 3 * LANES
    dma = pltpu.SemaphoreType.DMA
    half, full = jnp.bfloat16, jnp.float32
    return pl.pallas_call(
        functools.partial(fused_kernel, span, groups, escale, gscale),
        out_shape=(
            pltpu.VMEM((wl, quarter, width), full),
            pltpu.VMEM((1, wl), full),
        ),
        in_specs=[ANY, ANY],
        out_specs=(pl.BlockSpec(memory_space=pltpu.VMEM), pl.BlockSpec(memory_space=pltpu.VMEM)),
        scratch_shapes=[
            pltpu.VMEM((span, kept, mb, width), half),
            pltpu.VMEM((span, chunks, mb, 2 * cell), half),
            pltpu.VMEM((chunks, span * CORES, mb, 2 * cell), half),
            pltpu.VMEM((3 * span, m, LANES), half),
            pltpu.VMEM((3 * span, LANES, m), half),
            pltpu.VMEM((cell, 2 * cell), half),
            pltpu.VMEM((2 * cell, cell), half),
            pltpu.VMEM((3 * span, m, LANES), full),
            pltpu.VMEM((span, 2, 3, 3, quarter // 2, LANES), half),
            pltpu.VMEM((span, 2, 3, 3, quarter // 2, LANES), half),
            pltpu.VMEM((span, 2, 3, quarter // 2, LANES), half),
            pltpu.VMEM((span, 2, 3, quarter // 2, LANES), half),
            pltpu.VMEM((groups, 3, quarter // 2, LANES), half),
            pltpu.VMEM((groups, 3, quarter // 2, LANES), half),
            pltpu.VMEM((span + 1, wl, LANES), full),
            pltpu.VMEM((count, wl, LANES), full),
            dma((span + 2 * wl,)),
            dma((chunks, span)), dma((chunks, span)), dma((chunks, span)), dma((chunks, span)),
            dma((span,)), dma((span,)), dma((span, groups)), dma((span, groups)),
            dma((span, 2, 3)), dma((span, 2, 3)), dma((1,)), dma((1,)), dma((span, 2)), dma((span, 2)), dma((count,)), dma((count,)),
        ],
        compiler_params=pltpu.CompilerParams(collective_id=2, has_side_effects=True, vmem_limit_bytes=60 * 2**20),
    )(chol, jnp.swapaxes(green, 1, 2))


def fits(span, groups, chol, green):
    kl, mb, width = chol.shape
    wl, m, _ = green.shape
    powers = span & (span - 1) == 0 and groups & (groups - 1) == 0
    tiles = width == LANES + HALF and wl == 2 and mb % 16 == 0 and m % 64 == 0 and m % (groups * 32) == 0
    return powers and tiles and span == 4 and groups == 4 and kl % (span * BATCH) == 0 and span * m * width <= 2**21


def per_device(span, groups, chol_vectors, green):
    kl, mb, width = chol_vectors.shape
    wl, m, _ = green.shape
    nchol = kl * groups
    escale = 1.0 / (nchol * width)
    gscale = 1.0 / nchol**0.5
    chip, group = lax.axis_index("walker") // CORES, lax.axis_index("chol")

    if fits(span, groups, chol_vectors, green):
        gradient, energy = fused(span, groups, escale, gscale, chol_vectors, green)
        return energy[0], gradient

    blocks, greens = gather(span, groups, chol_vectors, green)
    chol = jnp.transpose(blocks, (1, 0, 2, 3)).reshape(kl // span, m, width)
    terms, lines = products(chol, greens.reshape(span * wl, m, width))

    sums = jnp.sum(lines, axis=(1, 2)).reshape(span, wl, 1)
    sums = jnp.broadcast_to(sums, (span, wl, 128))
    parts, energies = spread(span, groups, terms, sums)
    own = lax.dynamic_slice(terms, (chip * wl, group * (m // groups), 0), (wl, m // groups, width))
    gradient = (own.astype(jnp.float32) + jnp.sum(parts.astype(jnp.float32), axis=0)) * gscale
    energy = lax.dynamic_index_in_dim(sums, chip, 0, keepdims=False) + jnp.sum(energies, axis=0)
    return energy[:, 0] * escale, gradient


def solution(mesh):
    span, groups = mesh.shape["walker"] // CORES, mesh.shape["chol"]
    return jax.shard_map(
        functools.partial(per_device, span, groups),
        mesh=mesh,
        in_specs=(P("chol", "walker", None), P("walker", None, None)),
        out_specs=(P("walker"), P("walker", "chol", None)),
        check_vma=False,
    )
```
